256 devices in a mesh: lat: 32 (over z, x_hi, core), lon: 8 (over y, x_lo).
Axes of the slice: x: 4 (x_hi: 2, x_lo: 2; x = x_hi * 2 + x_lo), y: 4, z: 8, core: 2. Of those that a mesh axis runs over, the one named last changes fastest.
Arguments:
- elevation: float32 [8192, 16384], P('lat', 'lon'), may hold values from -200 to 200
Outputs:
- slope_angle: float32 [8192, 16384], P('lat', 'lon')
- facing: float32 [2, 8192, 16384], P(None, 'lat', 'lon')
- hillshade: float32 [8192, 16384], P('lat', 'lon')
The draws below stay inside these ranges and needn't reach their ends.
All inputs are finite; a program needn't handle non-finite values.
Results may differ from the reference program's by a relative error of at most 0.0003.
Values sent between devices are 32-bit elements; how exact they have to be, the bound alone decides.
A program may use at most 64 MiB of HBM per device.

```python
import math
import jax
import jax.numpy as jnp
from jax import lax

SCALES = 7
HALO = 64
NROWS = 8192
NCOLS = 16384


def draw_elevation(key, part):
    surface = jnp.zeros((NROWS, NCOLS), jnp.float32)
    for octave in range(SCALES):
        stride = 2 ** octave
        noise_key = jax.random.fold_in(key, 11 + octave)
        shift_key = jax.random.fold_in(key, 101 + octave)
        coarse_shape = (NROWS // stride, NCOLS // stride)
        coarse = jax.random.truncated_normal(noise_key, -4.0, 4.0, coarse_shape, jnp.float32)
        amplitude = 2.0 * math.sqrt(stride)
        upsampled = jnp.repeat(jnp.repeat(coarse, stride, axis=0), stride, axis=1)
        offsets = jax.random.randint(shift_key, (2,), 0, stride)
        upsampled = jnp.roll(upsampled, (offsets[0], offsets[1]), axis=(0, 1))
        surface = surface + amplitude * upsampled
    return surface


def setup_inputs(seed: int = 0) -> dict:
    streams_of = jax.random.split(jax.random.key(seed), 2)
    elevation = draw_elevation(jax.random.fold_in(streams_of[1], 71), 0)
    return dict(elevation=elevation)


LIGHT_EAST = -0.5
LIGHT_NORTH = 0.5
LIGHT_UP = math.sqrt(0.5)

def window(padded, margin, row_offset, col_offset, row_count, col_count):
    return lax.slice(padded, (margin + row_offset, margin + col_offset), (margin + row_offset + row_count, margin + col_offset + col_count))

def terrain_shading(padded, spacing, margin, levels):
    row_count = padded.shape[0] - 2 * margin
    col_count = padded.shape[1] - 2 * margin
    eastward = jnp.zeros((row_count, col_count), jnp.float32)
    northward = jnp.zeros((row_count, col_count), jnp.float32)
    for octave in range(levels):
        stride = 2 ** octave
        north_west = window(padded, margin, -stride, -stride, row_count, col_count)
        north_mid = window(padded, margin, -stride, 0, row_count, col_count)
        north_east = window(padded, margin, -stride, stride, row_count, col_count)
        west_mid = window(padded, margin, 0, -stride, row_count, col_count)
        east_mid = window(padded, margin, 0, stride, row_count, col_count)
        south_west = window(padded, margin, stride, -stride, row_count, col_count)
        south_mid = window(padded, margin, stride, 0, row_count, col_count)
        south_east = window(padded, margin, stride, stride, row_count, col_count)
        east_diff = north_east + 2.0 * east_mid + south_east - (north_west + 2.0 * west_mid + south_west)
        north_diff = north_west + 2.0 * north_mid + north_east - (south_west + 2.0 * south_mid + south_east)
        eastward = eastward + east_diff * (1.0 / stride)
        northward = northward + north_diff * (1.0 / stride)
    grad_east = eastward / (8.0 * levels * spacing[:, None])
    grad_north = northward * (1.0 / (8.0 * levels))
    squared = grad_east * grad_east + grad_north * grad_north
    slope_angle = jnp.arctan(jnp.sqrt(squared))
    inverse = lax.rsqrt(1.0 + squared)
    facing_east = -grad_east * inverse
    facing_north = -grad_north * inverse
    shading = jnp.maximum(LIGHT_EAST * facing_east + LIGHT_NORTH * facing_north + LIGHT_UP * inverse, 0.0)
    return (slope_angle, jnp.stack([facing_east, facing_north]), shading)

def reference(elevation):
    margin = HALO
    wrapped = jnp.concatenate([elevation[:, NCOLS - margin:], elevation, elevation[:, :margin]], axis=1)
    padded = jnp.concatenate([jnp.broadcast_to(wrapped[:1], (margin, NCOLS + 2 * margin)), wrapped, jnp.broadcast_to(wrapped[NROWS - 1:], (margin, NCOLS + 2 * margin))], axis=0)
    position = jnp.arange(NROWS, dtype=jnp.int32)
    spacing = jnp.sin((position.astype(jnp.float32) + 0.5) * (math.pi / NROWS)) * (2.0 * NROWS / NCOLS)
    block_rows = math.gcd(NROWS, 512)
    block_count = NROWS // block_rows

    def one_block(number):
        first_row = (number * block_rows).astype(jnp.int32)
        slab = lax.dynamic_slice(padded, (first_row, jnp.int32(0)), (block_rows + 2 * margin, NCOLS + 2 * margin))
        slab_spacing = lax.dynamic_slice(spacing, (first_row,), (block_rows,))
        return terrain_shading(slab, slab_spacing, margin, SCALES)
    results = lax.map(one_block, jnp.arange(block_count, dtype=jnp.int32))
    slope_angle = results[0].reshape(NROWS, NCOLS)
    facing = jnp.transpose(results[1], (1, 0, 2, 3)).reshape(2, NROWS, NCOLS)
    hillshade = results[2].reshape(NROWS, NCOLS)
    return (slope_angle, facing, hillshade)
```

```python
import math

import jax
import jax.numpy as jnp
from jax import lax
from jax.experimental import pallas as pl
from jax.experimental.pallas import tpu as pltpu
from jax.sharding import PartitionSpec as P


HALO = 64
LAGS = (1, 2, 4, 8, 16, 32, 64)
F32 = jnp.float32
ROWS, COLS, TILES = 256, 2048, 16


def pad_of(s):
    return max(8, s)


def shade(east, north, east_scale):
    grad_east = east * east_scale
    grad_north = north * (1.0 / 56.0)
    squared = grad_east * grad_east + grad_north * grad_north
    inverse = lax.rsqrt(1.0 + squared)
    a = jnp.sqrt(squared) * inverse
    b = 1.0 + inverse
    upper = a > 0.41421356 * b
    v = jnp.where(upper, a - b, a) / jnp.where(upper, a + b, b)
    z = v * v
    poly = ((8.05374449538e-2 * z - 1.38776856032e-1) * z + 1.99777106478e-1) * z - 3.33329491539e-1
    slope = 2.0 * (poly * z * v + v + jnp.where(upper, math.pi / 4, 0.0))
    facing_east = -grad_east * inverse
    facing_north = -grad_north * inverse
    shading = jnp.maximum(0.5 * (facing_north - facing_east) + math.sqrt(0.5) * inverse, 0.0)
    return slope, facing_east, facing_north, shading


def differences(z, lags):
    lane = lax.broadcasted_iota(jnp.int32, (8, 128), 1)
    out = {}
    for s in lags:
        right = [pltpu.roll(t, s, 1) for t in z[:-1]]
        if s == 64:
            left = [pltpu.roll(z[-1], 64, 1)]
            left = right[1:] + left
        else:
            left = [pltpu.roll(t, 128 - s, 1) for t in z[1:]]
        p, q = [], []
        for j in range(len(z) - 2):
            west = jnp.where(lane < s, right[j], right[j + 1])
            east = jnp.where(lane < 128 - s, left[j], left[j + 1])
            p.append((east - west) * (1.0 / s))
            q.append((east + west + 2.0 * z[j + 1]) * (1.0 / s))
        out[s] = (p, q)
    return out


def inner_kernel(x, wp, ep, gs, en, o_s, o_f, o_h, zc, ps, qs, cs, stage, sem_in, sem_out):
    loads = [
        pltpu.make_async_copy(
            x.at[pl.ds(64 * k, 64), pl.ds(128 * j, 128)],
            zc.at[j + 1, pl.ds(64 * k, 64)],
            sem_in.at[k, j],
        )
        for k in range(4)
        for j in range(TILES)
    ]
    for c in loads:
        c.start()
    zc[0, 0:128, :] = pltpu.roll(wp[...], 64, 1)
    zc[0, 128:256, :] = wp[...]
    zc[17, 0:128, :] = ep[...]
    zc[17, 128:256, :] = pltpu.roll(ep[...], 64, 1)
    for k, s in enumerate(LAGS):
        m = pad_of(s)
        for ref in (ps[k], qs[k]):
            ref[:, 0:m, :] = jnp.zeros((TILES, m, 128), F32)
            ref[:, m + ROWS : m + ROWS + m, :] = jnp.zeros((TILES, m, 128), F32)
    for c in loads:
        c.wait()

    def first(row):
        z = [zc[j, pl.ds(row, 8), :] for j in range(TILES + 2)]
        d = differences(z, LAGS)
        for k, s in enumerate(LAGS):
            for j in range(TILES):
                ps[k][j, pl.ds(row + pad_of(s), 8), :] = d[s][0][j]
                qs[k][j, pl.ds(row + pad_of(s), 8), :] = d[s][1][j]
        for j in range(TILES):
            cs[j, pl.ds(row, 8), :] = 2.0 * sum(d[s][0][j] for s in LAGS)

    def second(row, j):
        east = cs[j, pl.ds(row, 8), :]
        north = None
        for k, s in enumerate(LAGS):
            m = pad_of(s)
            above, below = pl.ds(row + (m - s), 8), pl.ds(row + (m + s), 8)
            east = east + (ps[k][j, above, :] + ps[k][j, below, :])
            diff = qs[k][j, above, :] - qs[k][j, below, :]
            north = diff if north is None else north + diff
        return east, north

    def partial(row, side, to):
        for j in range(TILES):
            east, north = second(row, j)
            en[side, 0, j, pl.ds(to, 8), :] = east
            en[side, 1, j, pl.ds(to, 8), :] = north

    def out_copies(g):
        rows, at = pl.ds(pl.multiple_of(8 * g, 8), 8), pl.ds(pl.multiple_of(8 * g + 64, 8), 8)
        return [
            pltpu.make_async_copy(stage.at[0, rows], o_s.at[at], sem_out.at[0, g]),
            pltpu.make_async_copy(stage.at[1, rows], o_f.at[0, at], sem_out.at[1, g]),
            pltpu.make_async_copy(stage.at[2, rows], o_f.at[1, at], sem_out.at[2, g]),
            pltpu.make_async_copy(stage.at[3, rows], o_h.at[at], sem_out.at[3, g]),
        ]

    def loop(lo, hi, body):
        def step(i, carry):
            body(pl.multiple_of(8 * i, 8), i)
            return carry

        lax.fori_loop(lo, hi, step, 0)

    def with_top(row, i):
        first(row)
        partial(pl.multiple_of(row - 64, 8), 0, pl.multiple_of(row - 64, 8))

    def with_middle(row, i):
        first(row)
        here = pl.multiple_of(row - 64, 8)
        to = pl.multiple_of(row - 128, 8)
        scale = gs[pl.ds(here, 8), :]
        for j in range(TILES):
            east, north = second(here, j)
            for k, v in enumerate(shade(east, north, scale)):
                stage[k, pl.ds(to, 8), 128 * j : 128 * j + 128] = v
        for c in out_copies(i - 16):
            c.start()

    loop(0, 8, lambda row, i: first(row))
    loop(8, 16, with_top)
    loop(16, 32, with_middle)
    loop(24, 32, lambda row, i: partial(row, 1, pl.multiple_of(row - 192, 8)))

    def drain(g, carry):
        for c in out_copies(g):
            c.wait()
        return carry

    lax.fori_loop(0, 16, drain, 0)


def rim_kernel(
    lat, top, bottom, nw, ne, sw, se, own, wp, ep, gs, en, i_s, i_f, i_h,
    o_s, o_f, o_h, hz, pt, qt, stage, sem_out,
):
    del i_s, i_f, i_h
    sides = ((0, top, nw, ne), (1, bottom, sw, se))
    for side, mid, west, east in sides:
        pole = lat[0] == (0 if side == 0 else lat[1] - 1)

        @pl.when(jnp.logical_not(pole))
        def _(side=side, mid=mid, west=west, east=east):
            hz[side, 0] = west[...]
            hz[side, 17] = east[...]
            for j in range(TILES):
                hz[side, j + 1] = mid[:, 128 * j : 128 * j + 128]

        @pl.when(pole)
        def _(side=side):
            at = 0 if side == 0 else 7
            edge = 0 if side == 0 else 127
            turn_w = pltpu.roll(wp[8 * (edge // 8) : 8 * (edge // 8) + 8, :], 64, 1)
            turn_e = pltpu.roll(ep[8 * (edge // 8) : 8 * (edge // 8) + 8, :], 64, 1)
            straight_w = wp[edge : edge + 1, :]
            straight_e = ep[edge : edge + 1, :]
            w = turn_w[at : at + 1] if side == 0 else straight_w
            e = straight_e if side == 0 else turn_e[at : at + 1]
            hz[side, 0] = jnp.broadcast_to(w, (64, 128))
            hz[side, 17] = jnp.broadcast_to(e, (64, 128))
            for j in range(TILES):
                line = own[side, at : at + 1, 128 * j : 128 * j + 128]
                hz[side, j + 1] = jnp.broadcast_to(line, (64, 128))

    zero = jnp.zeros((TILES, 8, 128), F32)
    for k in range(3):
        for ref in (pt[k], qt[k]):
            ref[0, :, 8:16, :] = zero
            ref[1, :, 0:8, :] = zero

    for side in range(2):
        for h in range(8):
            near = 7 - h if side == 0 else h
            lags = tuple(s for s in LAGS if pad_of(s) > 8 * near)
            z = [hz[side, j, 8 * h : 8 * h + 8, :] for j in range(TILES + 2)]
            d = differences(z, lags)
            for k, s in enumerate(LAGS):
                if s not in lags:
                    continue
                if s < 8:
                    at = 0 if side == 0 else 8
                else:
                    at = 8 * h - (64 - s) if side == 0 else 8 * h
                for j in range(TILES):
                    pt[k][side, j, at : at + 8, :] = d[s][0][j]
                    qt[k][side, j, at : at + 8, :] = d[s][1][j]

    copies = []
    for side in range(2):
        for g in range(8):
            for j in range(TILES):
                east = en[side, 0, j, 8 * g : 8 * g + 8, :]
                north = en[side, 1, j, 8 * g : 8 * g + 8, :]
                for k, s in enumerate(LAGS):
                    if side == 0:
                        if s < 8 and g == 0:
                            at = 8 - s
                        elif s >= 8 and 8 * g < s:
                            at = 8 * g
                        else:
                            continue
                        east = east + pt[k][0, j, at : at + 8, :]
                        north = north + qt[k][0, j, at : at + 8, :]
                    else:
                        if s < 8 and g == 7:
                            at = s
                        elif s >= 8 and 8 * g + s >= 64:
                            at = 8 * g + s - 64
                        else:
                            continue
                        east = east + pt[k][1, j, at : at + 8, :]
                        north = north - qt[k][1, j, at : at + 8, :]
                row = 8 * g + 192 * side
                for k, v in enumerate(shade(east, north, gs[row : row + 8, :])):
                    stage[side, k, 8 * g : 8 * g + 8, 128 * j : 128 * j + 128] = v
            rows, at = pl.ds(8 * g, 8), pl.ds(8 * g + 192 * side, 8)
            now = [
                pltpu.make_async_copy(stage.at[side, 0, rows], o_s.at[at], sem_out.at[side, g, 0]),
                pltpu.make_async_copy(stage.at[side, 1, rows], o_f.at[0, at], sem_out.at[side, g, 1]),
                pltpu.make_async_copy(stage.at[side, 2, rows], o_f.at[1, at], sem_out.at[side, g, 2]),
                pltpu.make_async_copy(stage.at[side, 3, rows], o_h.at[at], sem_out.at[side, g, 3]),
            ]
            for c in now:
                c.start()
            copies += now
    for c in copies:
        c.wait()


def outputs():
    return [
        jax.ShapeDtypeStruct((ROWS, COLS), F32),
        jax.ShapeDtypeStruct((2, ROWS, COLS), F32),
        jax.ShapeDtypeStruct((ROWS, COLS), F32),
    ]


def local(x):
    n_lat, n_lon = lax.axis_size("lat"), lax.axis_size("lon")
    lat = lax.axis_index("lat")

    def shift(block, dlat, dlon):
        pairs = [
            (i * n_lon + k, (i + dlat) * n_lon + (k + dlon) % n_lon)
            for i in range(n_lat)
            for k in range(n_lon)
            if 0 <= i + dlat < n_lat
        ]
        return lax.ppermute(block, ("lat", "lon"), pairs)

    half = ROWS // 2
    wp = shift(jnp.concatenate([x[:half, -HALO:], x[half:, -HALO:]], 1), 0, 1)
    ep = shift(jnp.concatenate([x[:half, :HALO], x[half:, :HALO]], 1), 0, -1)
    top = shift(x[-HALO:], 1, 0)
    bottom = shift(x[:HALO], -1, 0)
    nw = shift(x[-HALO:, -128:], 1, 1)
    ne = shift(x[-HALO:, :128], 1, -1)
    sw = shift(x[:HALO, -128:], -1, 1)
    se = shift(x[:HALO, :128], -1, -1)

    position = lat * ROWS + lax.iota(jnp.int32, ROWS)
    total_rows, total_cols = ROWS * n_lat, COLS * n_lon
    spacing = jnp.sin((position.astype(F32) + 0.5) * (math.pi / total_rows)) * (2.0 * total_rows / total_cols)
    gs = jnp.broadcast_to((1.0 / (56.0 * spacing))[:, None], (ROWS, 128))

    anywhere = pl.BlockSpec(memory_space=pl.ANY)
    vmem = pl.BlockSpec(memory_space=pltpu.VMEM)
    smem = pl.BlockSpec(memory_space=pltpu.SMEM)
    columns = [pltpu.VMEM((TILES, ROWS + 2 * pad_of(s), 128), F32) for s in LAGS]
    en, o_s, o_f, o_h = pl.pallas_call(
        inner_kernel,
        out_shape=[jax.ShapeDtypeStruct((2, 2, TILES, HALO, 128), F32), *outputs()],
        in_specs=[anywhere, vmem, vmem, vmem],
        out_specs=[vmem, anywhere, anywhere, anywhere],
        scratch_shapes=[
            pltpu.VMEM((TILES + 2, ROWS, 128), F32),
            columns,
            columns,
            pltpu.VMEM((TILES, ROWS, 128), F32),
            pltpu.VMEM((4, ROWS // 2, COLS), F32),
            pltpu.SemaphoreType.DMA((4, TILES)),
            pltpu.SemaphoreType.DMA((4, 16)),
        ],
        compiler_params=pltpu.CompilerParams(vmem_limit_bytes=50 << 20),
        cost_estimate=pl.CostEstimate(flops=100_000_000, bytes_accessed=8 << 20, transcendentals=0),
        name="inner",
    )(x, wp, ep, gs)

    near = [pltpu.VMEM((2, TILES, pad_of(s) if s >= 8 else 16, 128), F32) for s in LAGS]
    own = jnp.stack([x[:8], x[-8:]])
    where = jnp.stack([lat, jnp.int32(n_lat)]).astype(jnp.int32)
    return tuple(
        pl.pallas_call(
            rim_kernel,
            out_shape=outputs(),
            in_specs=[smem] + [vmem] * 11 + [anywhere] * 3,
            out_specs=[anywhere] * 3,
            scratch_shapes=[
                pltpu.VMEM((2, TILES + 2, HALO, 128), F32),
                near,
                near,
                pltpu.VMEM((2, 4, HALO, COLS), F32),
                pltpu.SemaphoreType.DMA((2, 8, 4)),
            ],
            input_output_aliases={12: 0, 13: 1, 14: 2},
            compiler_params=pltpu.CompilerParams(vmem_limit_bytes=40 << 20),
            cost_estimate=pl.CostEstimate(flops=50_000_000, bytes_accessed=8 << 20, transcendentals=0),
            name="rim",
        )(where, top, bottom, nw, ne, sw, se, own, wp, ep, gs, en, o_s, o_f, o_h)
    )


def solution(mesh):
    in_specs = (P("lat", "lon"),)
    out_specs = (P("lat", "lon"), P(None, "lat", "lon"), P("lat", "lon"))
    return jax.shard_map(local, mesh=mesh, in_specs=in_specs, out_specs=out_specs, check_vma=False)
```

```python
import math

import jax
import jax.numpy as jnp
from jax import lax
from jax.experimental import pallas as pl
from jax.experimental.pallas import tpu as pltpu
from jax.sharding import PartitionSpec as P

HALO = 64
LAGS = (1, 2, 4, 8, 16, 32, 64)
F32 = jnp.float32
ROWS, COLS, TILES = 256, 2048, 16


def pad_of(s):
    return max(8, s)


def shade(east, north, east_scale):
    grad_east = east * east_scale
    grad_north = north * (1.0 / 56.0)
    squared = grad_east * grad_east + grad_north * grad_north
    inverse = lax.rsqrt(1.0 + squared)
    a = jnp.sqrt(squared) * inverse
    b = 1.0 + inverse
    upper = a > 0.41421356 * b
    v = jnp.where(upper, a - b, a) / jnp.where(upper, a + b, b)
    z = v * v
    poly = ((8.05374449538e-2 * z - 1.38776856032e-1) * z + 1.99777106478e-1) * z - 3.33329491539e-1
    slope = 2.0 * (poly * z * v + v + jnp.where(upper, math.pi / 4, 0.0))
    facing_east = -grad_east * inverse
    facing_north = -grad_north * inverse
    shading = jnp.maximum(0.5 * (facing_north - facing_east) + math.sqrt(0.5) * inverse, 0.0)
    return slope, facing_east, facing_north, shading


def differences(z, lags):
    lane = lax.broadcasted_iota(jnp.int32, (8, 128), 1)
    out = {}
    for s in lags:
        right = [pltpu.roll(t, s, 1) for t in z[:-1]]
        if s == 64:
            left = [pltpu.roll(z[-1], 64, 1)]
            left = right[1:] + left
        else:
            left = [pltpu.roll(t, 128 - s, 1) for t in z[1:]]
        p, q = [], []
        for j in range(len(z) - 2):
            west = jnp.where(lane < s, right[j], right[j + 1])
            east = jnp.where(lane < 128 - s, left[j], left[j + 1])
            p.append((east - west) * (1.0 / s))
            q.append((east + west + 2.0 * z[j + 1]) * (1.0 / s))
        out[s] = (p, q)
    return out


CHUNK = 4
CHUNKS = TILES // CHUNK
SPANS = ((0, 5), (5, 4), (9, 4), (13, 3))


def exchange_kernel(
    x, scales, o_s, o_f, o_h, gs, zc, hz, packed, arrived, ps, qs, cs, en, pt, qt, sem_in, sem_out, sem_got, sem_gs
):
    lat, lon = lax.axis_index("lat"), lax.axis_index("lon")
    n_lat, n_lon = lax.axis_size("lat"), lax.axis_size("lon")
    east, west = lax.rem(lon + 1, n_lon), lax.rem(lon + n_lon - 1, n_lon)
    has_north, has_south = lat > 0, lat < n_lat - 1

    def load(k, j):
        return pltpu.make_async_copy(
            x.at[pl.ds(64 * k, 64), pl.ds(128 * j, 128)], zc.at[j + 1, pl.ds(64 * k, 64)], sem_in.at[k, j]
        )

    edges = [load(k, j) for j in (0, TILES - 1) for k in range(4)]
    rims = [load(k, j) for k in (0, 3) for j in range(1, TILES - 1)]
    middle = [load(k, j) for k in (1, 2) for j in range(1, TILES - 1)]
    for c in edges + rims + middle:
        c.start()
    scale_copy = pltpu.make_async_copy(scales, gs, sem_gs)
    scale_copy.start()

    barrier = pltpu.get_barrier_semaphore()

    def greet(to_lat, to_lon):
        pl.semaphore_signal(
            barrier, inc=1, device_id={"lat": to_lat, "lon": to_lon}, device_id_type=pl.DeviceIdType.MESH
        )

    greet(lat, east)
    greet(lat, west)

    @pl.when(has_north)
    def _():
        for to in (lon, east, west):
            greet(lat - 1, to)

    @pl.when(has_south)
    def _():
        for to in (lon, east, west):
            greet(lat + 1, to)

    lane = lax.broadcasted_iota(jnp.int32, (128, 128), 1)
    for c in edges:
        c.wait()
    packed[0] = jnp.where(lane < 64, pltpu.roll(zc[16, 0:128, :], 64, 1), zc[16, 128:256, :])
    packed[1] = jnp.where(lane < 64, zc[1, 0:128, :], pltpu.roll(zc[1, 128:256, :], 64, 1))
    for c in rims:
        c.wait()

    def send(src, dst, k, to_lat, to_lon):
        return pltpu.make_async_remote_copy(
            src_ref=src,
            dst_ref=dst,
            send_sem=sem_out.at[k],
            recv_sem=sem_got.at[k],
            device_id={"lat": to_lat, "lon": to_lon},
            device_id_type=pl.DeviceIdType.MESH,
        )

    first_rows, last_rows = pl.ds(0, 64), pl.ds(192, 64)
    along = [send(packed.at[0], arrived.at[0], 0, lat, east), send(packed.at[1], arrived.at[1], 1, lat, west)]
    south = [
        send(zc.at[16, last_rows], hz.at[0, 0], 2, lat + 1, east),
        send(zc.at[1, last_rows], hz.at[0, 17], 3, lat + 1, west),
    ]
    north = [
        send(zc.at[16, first_rows], hz.at[1, 0], 4, lat - 1, east),
        send(zc.at[1, first_rows], hz.at[1, 17], 5, lat - 1, west),
    ]
    for k, (at, n) in enumerate(SPANS):
        tiles = pl.ds(1 + at, n)
        south.append(send(zc.at[tiles, last_rows], hz.at[0, tiles], 6 + k, lat + 1, lon))
        north.append(send(zc.at[tiles, first_rows], hz.at[1, tiles], 10 + k, lat - 1, lon))

    inside = jnp.logical_and(has_north, has_south)
    pl.semaphore_wait(barrier, jnp.where(inside, 8, 5))
    for c in along:
        c.start()

    @pl.when(has_south)
    def _():
        for c in south:
            c.start()

    @pl.when(has_north)
    def _():
        for c in north:
            c.start()

    for k, s in enumerate(LAGS):
        m = pad_of(s)
        for ref in (ps[k], qs[k]):
            ref[:, 0:m, :] = jnp.zeros((TILES, m, 128), F32)
            ref[:, m + ROWS : m + ROWS + m, :] = jnp.zeros((TILES, m, 128), F32)
    zero = jnp.zeros((CHUNK, 8, 128), F32)
    for k in range(3):
        for ref in (pt[k], qt[k]):
            ref[0, :, 8:16, :] = zero
            ref[1, :, 0:8, :] = zero
    for c in middle:
        c.wait()
    scale_copy.wait()
    for c in along:
        c.wait()
    zc[0, 0:128, :] = pltpu.roll(arrived[0], 64, 1)
    zc[0, 128:256, :] = arrived[0]
    zc[17, 0:128, :] = arrived[1]
    zc[17, 128:256, :] = pltpu.roll(arrived[1], 64, 1)

    def first(row):
        z = [zc[j, pl.ds(row, 8), :] for j in range(TILES + 2)]
        d = differences(z, LAGS)
        for k, s in enumerate(LAGS):
            for j in range(TILES):
                ps[k][j, pl.ds(row + pad_of(s), 8), :] = d[s][0][j]
                qs[k][j, pl.ds(row + pad_of(s), 8), :] = d[s][1][j]
        for j in range(TILES):
            cs[j, pl.ds(row, 8), :] = 2.0 * sum(d[s][0][j] for s in LAGS)

    def second(row, j):
        to_east = cs[j, pl.ds(row, 8), :]
        to_north = None
        for k, s in enumerate(LAGS):
            m = pad_of(s)
            above, below = pl.ds(row + (m - s), 8), pl.ds(row + (m + s), 8)
            to_east = to_east + (ps[k][j, above, :] + ps[k][j, below, :])
            diff = qs[k][j, above, :] - qs[k][j, below, :]
            to_north = diff if to_north is None else to_north + diff
        return to_east, to_north

    def partial(row, side, to):
        for j in range(TILES):
            to_east, to_north = second(row, j)
            en[side, 0, j, pl.ds(to, 8), :] = to_east
            en[side, 1, j, pl.ds(to, 8), :] = to_north

    def put(rows, columns, values):
        o_s[rows, columns] = values[0]
        o_f[0, rows, columns] = values[1]
        o_f[1, rows, columns] = values[2]
        o_h[rows, columns] = values[3]

    def loop(lo, hi, body):
        def step(i, carry):
            body(pl.multiple_of(8 * i, 8))
            return carry

        lax.fori_loop(lo, hi, step, 0)

    def with_top(row):
        first(row)
        partial(pl.multiple_of(row - 64, 8), 0, pl.multiple_of(row - 64, 8))

    def with_middle(row):
        first(row)
        here = pl.multiple_of(row - 64, 8)
        scale = gs[pl.ds(here, 8), :]
        for j in range(TILES):
            put(pl.ds(here, 8), pl.ds(128 * j, 128), shade(*second(here, j), scale))

    loop(0, 8, first)
    loop(8, 16, with_top)
    loop(16, 32, with_middle)
    loop(24, 32, lambda row: partial(row, 1, pl.multiple_of(row - 192, 8)))

    def clamp(side):
        row = 0 if side == 0 else ROWS - 1
        for j in range(TILES + 2):
            hz[side, j] = jnp.broadcast_to(zc[j, row : row + 1, :], (64, 128))

    @pl.when(has_south)
    def _():
        for c in south:
            c.wait_send()
        for c in north[:2]:
            c.wait_recv()

    @pl.when(has_north)
    def _():
        for c in north:
            c.wait_send()
        for c in south[:2]:
            c.wait_recv()

    @pl.when(jnp.logical_not(has_north))
    def _():
        clamp(0)

    @pl.when(jnp.logical_not(has_south))
    def _():
        clamp(1)

    for b in range(CHUNKS):

        @pl.when(has_south)
        def _(b=b):
            north[2 + b].wait_recv()

        @pl.when(has_north)
        def _(b=b):
            south[2 + b].wait_recv()

        rim(b * CHUNK, hz, pt, qt, en, gs, put)


def rim(t0, hz, pt, qt, en, gs, put):
    for side in range(2):
        for h in range(8):
            near = 7 - h if side == 0 else h
            lags = tuple(s for s in LAGS if pad_of(s) > 8 * near)
            z = [hz[side, t0 + j, 8 * h : 8 * h + 8, :] for j in range(CHUNK + 2)]
            d = differences(z, lags)
            for k, s in enumerate(LAGS):
                if s not in lags:
                    continue
                if s < 8:
                    at = 0 if side == 0 else 8
                else:
                    at = 8 * h - (64 - s) if side == 0 else 8 * h
                for j in range(CHUNK):
                    pt[k][side, j, at : at + 8, :] = d[s][0][j]
                    qt[k][side, j, at : at + 8, :] = d[s][1][j]
        for g in range(8):
            for j in range(CHUNK):
                to_east = en[side, 0, t0 + j, 8 * g : 8 * g + 8, :]
                to_north = en[side, 1, t0 + j, 8 * g : 8 * g + 8, :]
                for k, s in enumerate(LAGS):
                    if side == 0:
                        if s < 8 and g == 0:
                            at = 8 - s
                        elif s >= 8 and 8 * g < s:
                            at = 8 * g
                        else:
                            continue
                        to_east = to_east + pt[k][0, j, at : at + 8, :]
                        to_north = to_north + qt[k][0, j, at : at + 8, :]
                    else:
                        if s < 8 and g == 7:
                            at = s
                        elif s >= 8 and 8 * g + s >= 64:
                            at = 8 * g + s - 64
                        else:
                            continue
                        to_east = to_east + pt[k][1, j, at : at + 8, :]
                        to_north = to_north - qt[k][1, j, at : at + 8, :]
                row = 8 * g + 192 * side
                columns = pl.ds(128 * (t0 + j), 128)
                put(pl.ds(row, 8), columns, shade(to_east, to_north, gs[row : row + 8, :]))


def store_kernel(i_s, i_f, i_h, o_s, o_f, o_h, sem):
    copies = []
    for k in range(4):
        rows = pl.ds(64 * k, 64)
        copies += [
            pltpu.make_async_copy(i_s.at[rows], o_s.at[rows], sem.at[0, k]),
            pltpu.make_async_copy(i_f.at[0, rows], o_f.at[0, rows], sem.at[1, k]),
            pltpu.make_async_copy(i_f.at[1, rows], o_f.at[1, rows], sem.at[2, k]),
            pltpu.make_async_copy(i_h.at[rows], o_h.at[rows], sem.at[3, k]),
        ]
    for c in copies:
        c.start()
    for c in copies:
        c.wait()


OUTPUTS = ((ROWS, COLS), (2, ROWS, COLS), (ROWS, COLS))


def local(x):
    n_lat, n_lon = lax.axis_size("lat"), lax.axis_size("lon")
    position = lax.axis_index("lat") * ROWS + lax.iota(jnp.int32, ROWS)
    total_rows, total_cols = ROWS * n_lat, COLS * n_lon
    spacing = jnp.sin((position.astype(F32) + 0.5) * (math.pi / total_rows)) * (2.0 * total_rows / total_cols)
    gs = jnp.broadcast_to((1.0 / (56.0 * spacing))[:, None], (ROWS, 128))

    anywhere = pl.BlockSpec(memory_space=pl.ANY)
    vmem = pl.BlockSpec(memory_space=pltpu.VMEM)
    columns = [pltpu.VMEM((TILES, ROWS + 2 * pad_of(s), 128), F32) for s in LAGS]
    near = [pltpu.VMEM((2, CHUNK, pad_of(s) if s >= 8 else 16, 128), F32) for s in LAGS]
    results = pl.pallas_call(
        exchange_kernel,
        out_shape=[pltpu.VMEM(shape, F32) for shape in OUTPUTS],
        in_specs=[pl.BlockSpec(memory_space=pltpu.HBM)] * 2,
        out_specs=[vmem] * 3,
        scratch_shapes=[
            pltpu.VMEM((ROWS, 128), F32),
            pltpu.VMEM((TILES + 2, ROWS, 128), F32),
            pltpu.VMEM((2, TILES + 2, HALO, 128), F32),
            pltpu.VMEM((2, 128, 128), F32),
            pltpu.VMEM((2, 128, 128), F32),
            columns,
            columns,
            pltpu.VMEM((TILES, ROWS, 128), F32),
            pltpu.VMEM((2, 2, TILES, HALO, 128), F32),
            near,
            near,
            pltpu.SemaphoreType.DMA((4, TILES)),
            pltpu.SemaphoreType.DMA((14,)),
            pltpu.SemaphoreType.DMA((14,)),
            pltpu.SemaphoreType.DMA,
        ],
        compiler_params=pltpu.CompilerParams(collective_id=0, has_side_effects=True, vmem_limit_bytes=46 << 20),
        name="exchange",
    )(x, gs)
    return tuple(
        pl.pallas_call(
            store_kernel,
            out_shape=[jax.ShapeDtypeStruct(shape, F32) for shape in OUTPUTS],
            in_specs=[vmem] * 3,
            out_specs=[anywhere] * 3,
            scratch_shapes=[pltpu.SemaphoreType.DMA((4, 4))],
            compiler_params=pltpu.CompilerParams(vmem_limit_bytes=16 << 20),
            name="store",
        )(*results)
    )


def solution(mesh):
    in_specs = (P("lat", "lon"),)
    out_specs = (P("lat", "lon"), P(None, "lat", "lon"), P("lat", "lon"))
    return jax.shard_map(local, mesh=mesh, in_specs=in_specs, out_specs=out_specs, check_vma=False)
```

```python
import math

import jax
import jax.numpy as jnp
from jax import lax
from jax.experimental import pallas as pl
from jax.experimental.pallas import tpu as pltpu
from jax.sharding import PartitionSpec as P

HALO = 64
LAGS = (1, 2, 4, 8, 16, 32, 64)
F32 = jnp.float32
ROWS, COLS, TILES = 256, 2048, 16


def pad_of(s):
    return max(8, s)


SMALLEST = 1.1754944e-38


def shade(east, north, east_scale):
    grad_east = east * east_scale
    grad_north = north * (1.0 / 56.0)
    squared = grad_east * grad_east + grad_north * grad_north
    inverse = lax.rsqrt(1.0 + squared)
    a = squared * lax.rsqrt(jnp.maximum(squared, SMALLEST)) * inverse
    b = 1.0 + inverse
    upper = a > 0.41421356 * b
    v = jnp.where(upper, a - b, a) / jnp.where(upper, a + b, b)
    z = v * v
    poly = ((2 * 8.05374449538e-2 * z - 2 * 1.38776856032e-1) * z + 2 * 1.99777106478e-1) * z - 2 * 3.33329491539e-1
    slope = (poly * z + 2.0) * v + jnp.where(upper, math.pi / 2, 0.0)
    down = -inverse
    facing_east = grad_east * down
    facing_north = grad_north * down
    shading = jnp.maximum((0.5 * (grad_east - grad_north) + math.sqrt(0.5)) * inverse, 0.0)
    return slope, facing_east, facing_north, shading


def differences(tiles, count, lags):
    lane = lax.broadcasted_iota(jnp.int32, (8, 128), 1)
    scaled, right, left = {}, {}, {}

    def at(j, s):
        if (j, s) not in scaled:
            if s == 0.5:
                scaled[j, s] = 2.0 * at(j, 1)
            elif s == 1:
                scaled[j, s] = tiles(j)
            else:
                scaled[j, s] = at(j, 1) * (1.0 / s)
        return scaled[j, s]

    def turned(j, s):
        if (j, s) not in right:
            right[j, s] = pltpu.roll(at(j, s), s, 1)
        return right[j, s]

    def turned_back(j, s):
        if s == 64:
            return turned(j, s)
        if (j, s) not in left:
            left[j, s] = pltpu.roll(at(j, s), 128 - s, 1)
        return left[j, s]

    for j in range(count):
        out = {}
        for s in lags:
            west = jnp.where(lane < s, turned(j, s), turned(j + 1, s))
            east = jnp.where(lane < 128 - s, turned_back(j + 1, s), turned_back(j + 2, s))
            out[s] = (east - west, east + west + at(j + 1, s / 2 if s > 1 else 0.5))
        yield j, out


CHUNK = 4
CHUNKS = TILES // CHUNK
SPANS = ((0, 5), (5, 4), (9, 4), (13, 3))


def exchange_kernel(
    x, o_s, o_f, o_h, gs, zc, hz, packed, arrived, ps, qs, cs, en, pt, qt, sem_in, sem_out, sem_got
):
    lat, lon = lax.axis_index("lat"), lax.axis_index("lon")
    n_lat, n_lon = lax.axis_size("lat"), lax.axis_size("lon")
    east, west = lax.rem(lon + 1, n_lon), lax.rem(lon + n_lon - 1, n_lon)
    has_north, has_south = lat > 0, lat < n_lat - 1

    def load(k, j):
        return pltpu.make_async_copy(
            x.at[pl.ds(64 * k, 64), pl.ds(128 * j, 128)], zc.at[j + 1, pl.ds(64 * k, 64)], sem_in.at[k, j]
        )

    edges = [load(k, j) for j in (0, TILES - 1) for k in range(4)]
    rims = [load(k, j) for k in (0, 3) for j in range(1, TILES - 1)]
    middle = [load(k, j) for k in (1, 2) for j in range(1, TILES - 1)]
    for c in edges + rims + middle:
        c.start()

    barrier = pltpu.get_barrier_semaphore()

    def greet(to_lat, to_lon):
        pl.semaphore_signal(
            barrier, inc=1, device_id={"lat": to_lat, "lon": to_lon}, device_id_type=pl.DeviceIdType.MESH
        )

    greet(lat, east)
    greet(lat, west)

    @pl.when(has_north)
    def _():
        for to in (lon, east, west):
            greet(lat - 1, to)

    @pl.when(has_south)
    def _():
        for to in (lon, east, west):
            greet(lat + 1, to)

    total_rows, total_cols = ROWS * n_lat, COLS * n_lon
    position = (lat * ROWS + lax.broadcasted_iota(jnp.int32, (ROWS, 128), 0)).astype(F32)
    spacing = jnp.sin((position + 0.5) * (math.pi / total_rows)) * (2.0 * total_rows / total_cols)
    gs[...] = 1.0 / (56.0 * spacing)
    for k, s in enumerate(LAGS):
        m = pad_of(s)
        for ref in (ps[k], qs[k]):
            ref[:, 0:m, :] = jnp.zeros((TILES, m, 128), F32)
            ref[:, m + ROWS : m + ROWS + m, :] = jnp.zeros((TILES, m, 128), F32)
    zero = jnp.zeros((CHUNK, 8, 128), F32)
    for k in range(3):
        for ref in (pt[k], qt[k]):
            ref[0, :, 8:16, :] = zero
            ref[1, :, 0:8, :] = zero
    lane = lax.broadcasted_iota(jnp.int32, (128, 128), 1)
    for c in edges:
        c.wait()
    packed[0] = jnp.where(lane < 64, pltpu.roll(zc[16, 0:128, :], 64, 1), zc[16, 128:256, :])
    packed[1] = jnp.where(lane < 64, zc[1, 0:128, :], pltpu.roll(zc[1, 128:256, :], 64, 1))
    for c in rims:
        c.wait()

    def send(src, dst, k, to_lat, to_lon):
        return pltpu.make_async_remote_copy(
            src_ref=src,
            dst_ref=dst,
            send_sem=sem_out.at[k],
            recv_sem=sem_got.at[k],
            device_id={"lat": to_lat, "lon": to_lon},
            device_id_type=pl.DeviceIdType.MESH,
        )

    first_rows, last_rows = pl.ds(0, 64), pl.ds(192, 64)
    along = [send(packed.at[0], arrived.at[0], 0, lat, east), send(packed.at[1], arrived.at[1], 1, lat, west)]
    south = [
        send(zc.at[16, last_rows], hz.at[0, 0], 2, lat + 1, east),
        send(zc.at[1, last_rows], hz.at[0, 17], 3, lat + 1, west),
    ]
    north = [
        send(zc.at[16, first_rows], hz.at[1, 0], 4, lat - 1, east),
        send(zc.at[1, first_rows], hz.at[1, 17], 5, lat - 1, west),
    ]
    for k, (at, n) in enumerate(SPANS):
        tiles = pl.ds(1 + at, n)
        south.append(send(zc.at[tiles, last_rows], hz.at[0, tiles], 6 + k, lat + 1, lon))
        north.append(send(zc.at[tiles, first_rows], hz.at[1, tiles], 10 + k, lat - 1, lon))

    inside = jnp.logical_and(has_north, has_south)
    pl.semaphore_wait(barrier, jnp.where(inside, 8, 5))
    for c in along:
        c.start()

    @pl.when(has_south)
    def _():
        for c in south:
            c.start()

    @pl.when(has_north)
    def _():
        for c in north:
            c.start()

    for c in middle:
        c.wait()

    def first(row, t0=0, count=TILES):
        for i, d in differences(lambda j: zc[t0 + j, pl.ds(row, 8), :], count, LAGS):
            j = t0 + i
            total = None
            for k, s in enumerate(LAGS):
                ps[k][j, pl.ds(row + pad_of(s), 8), :] = d[s][0]
                qs[k][j, pl.ds(row + pad_of(s), 8), :] = d[s][1]
                total = d[s][0] if total is None else total + d[s][0]
            cs[j, pl.ds(row, 8), :] = 2.0 * total

    def second(row, j):
        to_east = cs[j, pl.ds(row, 8), :]
        to_north = None
        for k, s in enumerate(LAGS):
            m = pad_of(s)
            above, below = pl.ds(row + (m - s), 8), pl.ds(row + (m + s), 8)
            to_east = to_east + (ps[k][j, above, :] + ps[k][j, below, :])
            diff = qs[k][j, above, :] - qs[k][j, below, :]
            to_north = diff if to_north is None else to_north + diff
        return to_east, to_north

    def put(rows, columns, values):
        o_s[rows, columns] = values[0]
        o_f[0, rows, columns] = values[1]
        o_f[1, rows, columns] = values[2]
        o_h[rows, columns] = values[3]

    def partial(row, side, to, tiles):
        for j in tiles:
            to_east, to_north = second(row, j)
            en[side, 0, j, pl.ds(to, 8), :] = to_east
            en[side, 1, j, pl.ds(to, 8), :] = to_north

    def finish(row, tiles):
        scale = gs[pl.ds(row, 8), :]
        for j in tiles:
            put(pl.ds(row, 8), pl.ds(128 * j, 128), shade(*second(row, j), scale))

    def loop(lo, hi, body):
        def step(i, carry):
            body(pl.multiple_of(8 * i, 8))
            return carry

        lax.fori_loop(lo, hi, step, 0)

    def back(row, by):
        return pl.multiple_of(row - by, 8)

    inner = range(1, TILES - 1)

    def with_top(row):
        first(row, 1, TILES - 2)
        partial(back(row, 64), 0, back(row, 64), inner)

    def with_middle(row):
        first(row, 1, TILES - 2)
        finish(back(row, 64), inner)

    loop(0, 8, lambda row: first(row, 1, TILES - 2))
    loop(8, 16, with_top)
    loop(16, 32, with_middle)
    loop(24, 32, lambda row: partial(row, 1, back(row, 192), inner))

    for c in along:
        c.wait()
    zc[0, 0:128, :] = pltpu.roll(arrived[0], 64, 1)
    zc[0, 128:256, :] = arrived[0]
    zc[17, 0:128, :] = arrived[1]
    zc[17, 128:256, :] = pltpu.roll(arrived[1], 64, 1)

    outer = (0, TILES - 1)

    def ends(row):
        for r in range(4):
            for j in outer:
                first(row * 4 + 8 * r, j, 1)

    def ends_rims(row):
        partial(row, 0, row, outer)
        partial(row + 192, 1, row, outer)

    def ends_middle(row):
        for r in range(4):
            finish(64 + row * 4 + 8 * r, outer)

    loop(0, 8, ends)
    loop(0, 8, ends_rims)
    loop(0, 4, ends_middle)

    def clamp(side):
        row = 0 if side == 0 else ROWS - 1
        for j in range(TILES + 2):
            hz[side, j] = jnp.broadcast_to(zc[j, row : row + 1, :], (64, 128))

    @pl.when(has_south)
    def _():
        for c in south:
            c.wait_send()
        for c in north[:2]:
            c.wait_recv()

    @pl.when(has_north)
    def _():
        for c in north:
            c.wait_send()
        for c in south[:2]:
            c.wait_recv()

    @pl.when(jnp.logical_not(has_north))
    def _():
        clamp(0)

    @pl.when(jnp.logical_not(has_south))
    def _():
        clamp(1)

    for b in range(CHUNKS):

        @pl.when(has_south)
        def _(b=b):
            north[2 + b].wait_recv()

        @pl.when(has_north)
        def _(b=b):
            south[2 + b].wait_recv()

        rim(b * CHUNK, hz, pt, qt, en, gs, put)


def rim(t0, hz, pt, qt, en, gs, put):
    for side in range(2):
        for h in range(8):
            near = 7 - h if side == 0 else h
            lags = tuple(s for s in LAGS if pad_of(s) > 8 * near)
            for j, d in differences(lambda j: hz[side, t0 + j, 8 * h : 8 * h + 8, :], CHUNK, lags):
                for s in lags:
                    if s < 8:
                        at = 0 if side == 0 else 8
                    else:
                        at = 8 * h - (64 - s) if side == 0 else 8 * h
                    pt[LAGS.index(s)][side, j, at : at + 8, :] = d[s][0]
                    qt[LAGS.index(s)][side, j, at : at + 8, :] = d[s][1]
        for g in range(8):
            for j in range(CHUNK):
                to_east = en[side, 0, t0 + j, 8 * g : 8 * g + 8, :]
                to_north = en[side, 1, t0 + j, 8 * g : 8 * g + 8, :]
                for k, s in enumerate(LAGS):
                    if side == 0:
                        if s < 8 and g == 0:
                            at = 8 - s
                        elif s >= 8 and 8 * g < s:
                            at = 8 * g
                        else:
                            continue
                        to_east = to_east + pt[k][0, j, at : at + 8, :]
                        to_north = to_north + qt[k][0, j, at : at + 8, :]
                    else:
                        if s < 8 and g == 7:
                            at = s
                        elif s >= 8 and 8 * g + s >= 64:
                            at = 8 * g + s - 64
                        else:
                            continue
                        to_east = to_east + pt[k][1, j, at : at + 8, :]
                        to_north = to_north - qt[k][1, j, at : at + 8, :]
                row = 8 * g + 192 * side
                columns = pl.ds(128 * (t0 + j), 128)
                put(pl.ds(row, 8), columns, shade(to_east, to_north, gs[row : row + 8, :]))


def store_kernel(i_s, i_f, i_h, o_s, o_f, o_h, sem):
    copies = []
    for k in range(4):
        rows = pl.ds(64 * k, 64)
        copies += [
            pltpu.make_async_copy(i_s.at[rows], o_s.at[rows], sem.at[0, k]),
            pltpu.make_async_copy(i_f.at[0, rows], o_f.at[0, rows], sem.at[1, k]),
            pltpu.make_async_copy(i_f.at[1, rows], o_f.at[1, rows], sem.at[2, k]),
            pltpu.make_async_copy(i_h.at[rows], o_h.at[rows], sem.at[3, k]),
        ]
    for c in copies:
        c.start()
    for c in copies:
        c.wait()


OUTPUTS = ((ROWS, COLS), (2, ROWS, COLS), (ROWS, COLS))


def local(x):
    anywhere = pl.BlockSpec(memory_space=pl.ANY)
    vmem = pl.BlockSpec(memory_space=pltpu.VMEM)
    columns = [pltpu.VMEM((TILES, ROWS + 2 * pad_of(s), 128), F32) for s in LAGS]
    near = [pltpu.VMEM((2, CHUNK, pad_of(s) if s >= 8 else 16, 128), F32) for s in LAGS]
    results = pl.pallas_call(
        exchange_kernel,
        out_shape=[pltpu.VMEM(shape, F32) for shape in OUTPUTS],
        in_specs=[pl.BlockSpec(memory_space=pltpu.HBM)],
        out_specs=[vmem] * 3,
        scratch_shapes=[
            pltpu.VMEM((ROWS, 128), F32),
            pltpu.VMEM((TILES + 2, ROWS, 128), F32),
            pltpu.VMEM((2, TILES + 2, HALO, 128), F32),
            pltpu.VMEM((2, 128, 128), F32),
            pltpu.VMEM((2, 128, 128), F32),
            columns,
            columns,
            pltpu.VMEM((TILES, ROWS, 128), F32),
            pltpu.VMEM((2, 2, TILES, HALO, 128), F32),
            near,
            near,
            pltpu.SemaphoreType.DMA((4, TILES)),
            pltpu.SemaphoreType.DMA((14,)),
            pltpu.SemaphoreType.DMA((14,)),
        ],
        compiler_params=pltpu.CompilerParams(collective_id=0, has_side_effects=True, vmem_limit_bytes=46 << 20),
        name="exchange",
    )(x)
    return tuple(
        pl.pallas_call(
            store_kernel,
            out_shape=[jax.ShapeDtypeStruct(shape, F32) for shape in OUTPUTS],
            in_specs=[vmem] * 3,
            out_specs=[anywhere] * 3,
            scratch_shapes=[pltpu.SemaphoreType.DMA((4, 4))],
            compiler_params=pltpu.CompilerParams(vmem_limit_bytes=16 << 20),
            name="store",
        )(*results)
    )


def solution(mesh):
    in_specs = (P("lat", "lon"),)
    out_specs = (P("lat", "lon"), P(None, "lat", "lon"), P("lat", "lon"))
    return jax.shard_map(local, mesh=mesh, in_specs=in_specs, out_specs=out_specs, check_vma=False)
```

```python
import math

import jax
import jax.numpy as jnp
from jax import lax
from jax.experimental import pallas as pl
from jax.experimental.pallas import tpu as pltpu
from jax.sharding import PartitionSpec as P

HALO = 64
LAGS = (1, 2, 4, 8, 16, 32, 64)
F32 = jnp.float32
ROWS, COLS, TILES = 256, 2048, 16


def pad_of(s):
    return max(8, s)


SMALLEST = 1.1754944e-38


def shade(east, north, east_scale):
    grad_east = east * east_scale
    grad_north = north * (1.0 / 56.0)
    squared = grad_east * grad_east + grad_north * grad_north
    inverse = lax.rsqrt(1.0 + squared)
    a = squared * lax.rsqrt(jnp.maximum(squared, SMALLEST)) * inverse
    b = 1.0 + inverse
    upper = a > 0.41421356 * b
    v = jnp.where(upper, a - b, a) / jnp.where(upper, a + b, b)
    z = v * v
    poly = ((2 * 8.05374449538e-2 * z - 2 * 1.38776856032e-1) * z + 2 * 1.99777106478e-1) * z - 2 * 3.33329491539e-1
    slope = (poly * z + 2.0) * v + jnp.where(upper, math.pi / 2, 0.0)
    down = -inverse
    facing_east = grad_east * down
    facing_north = grad_north * down
    shading = jnp.maximum((0.5 * (grad_east - grad_north) + math.sqrt(0.5)) * inverse, 0.0)
    return slope, facing_east, facing_north, shading


def differences(tiles, count, lags):
    lane = lax.broadcasted_iota(jnp.int32, (8, 128), 1)
    scaled, right, left = {}, {}, {}

    def at(j, s):
        if (j, s) not in scaled:
            if s == 0.5:
                scaled[j, s] = 2.0 * at(j, 1)
            elif s == 1:
                scaled[j, s] = tiles(j)
            else:
                scaled[j, s] = at(j, 1) * (1.0 / s)
        return scaled[j, s]

    def turned(j, s):
        if (j, s) not in right:
            right[j, s] = pltpu.roll(at(j, s), s, 1)
        return right[j, s]

    def turned_back(j, s):
        if s == 64:
            return turned(j, s)
        if (j, s) not in left:
            left[j, s] = pltpu.roll(at(j, s), 128 - s, 1)
        return left[j, s]

    for j in range(count):
        out = {}
        for s in lags:
            west = jnp.where(lane < s, turned(j, s), turned(j + 1, s))
            east = jnp.where(lane < 128 - s, turned_back(j + 1, s), turned_back(j + 2, s))
            out[s] = (east - west, east + west + at(j + 1, s / 2 if s > 1 else 0.5))
        yield j, out


BLOCKS = ((1, 4), (5, 4), (9, 4), (13, 2))
SPANS = ((0, 6), (6, 4), (10, 4), (14, 2))
MOST = 4
ENDS = (0, TILES - 1)


def clear(pt, qt):
    for k in range(3):
        for ref in (pt[k], qt[k]):
            zero = jnp.zeros((ref.shape[1], 8, 128), F32)
            ref[0, :, 8:16, :] = zero
            ref[1, :, 0:8, :] = zero


def halo_differences(side, tiles, at, count, pt, qt):
    for h in range(8):
        near = 7 - h if side == 0 else h
        lags = tuple(s for s in LAGS if pad_of(s) > 8 * near)
        for j, d in differences(lambda j, h=h: tiles(h, j), count, lags):
            for s in lags:
                if s < 8:
                    row = 0 if side == 0 else 8
                else:
                    row = 8 * h - (64 - s) if side == 0 else 8 * h
                k = LAGS.index(s)
                pt[k][side, at + j, row : row + 8, :] = d[s][0]
                qt[k][side, at + j, row : row + 8, :] = d[s][1]


def halo_sums(side, g, j, pt, qt, to_east, to_north):
    for k, s in enumerate(LAGS):
        if side == 0:
            if s < 8 and g == 0:
                row = 8 - s
            elif s >= 8 and 8 * g < s:
                row = 8 * g
            else:
                continue
            to_north = to_north + qt[k][0, j, row : row + 8, :]
        else:
            if s < 8 and g == 7:
                row = s
            elif s >= 8 and 8 * g + s >= 64:
                row = 8 * g + s - 64
            else:
                continue
            to_north = to_north - qt[k][1, j, row : row + 8, :]
        to_east = to_east + pt[k][side, j, row : row + 8, :]
    return to_east, to_north


def loop(lo, hi, body):
    def step(i, carry):
        body(pl.multiple_of(8 * i, 8))
        return carry

    lax.fori_loop(lo, hi, step, 0)


def exchange_kernel(
    x, o_s, o_f, o_h, hz, ends, gs, arrived, corners, zc, packed, ps, qs, cs, en, pt, qt, sem_in, sem_out, sem_got
):
    lat, lon = lax.axis_index("lat"), lax.axis_index("lon")
    n_lat, n_lon = lax.axis_size("lat"), lax.axis_size("lon")
    east, west = lax.rem(lon + 1, n_lon), lax.rem(lon + n_lon - 1, n_lon)
    has_north, has_south = lat > 0, lat < n_lat - 1

    def load(k, j):
        return pltpu.make_async_copy(
            x.at[pl.ds(64 * k, 64), pl.ds(128 * j, 128)], zc.at[j + 1, pl.ds(64 * k, 64)], sem_in.at[k, j]
        )

    rims = [load(k, j) for k in (0, 3) for j in range(TILES)]
    middle = [load(k, j) for k in (1, 2) for j in range(TILES)]
    for c in rims + middle:
        c.start()

    barrier = pltpu.get_barrier_semaphore()

    def greet(to_lat, to_lon):
        pl.semaphore_signal(
            barrier, inc=1, device_id={"lat": to_lat, "lon": to_lon}, device_id_type=pl.DeviceIdType.MESH
        )

    greet(lat, east)
    greet(lat, west)

    @pl.when(has_north)
    def _():
        for to in (lon, east, west):
            greet(lat - 1, to)

    @pl.when(has_south)
    def _():
        for to in (lon, east, west):
            greet(lat + 1, to)

    total_rows, total_cols = ROWS * n_lat, COLS * n_lon
    position = (lat * ROWS + lax.broadcasted_iota(jnp.int32, (ROWS, 128), 0)).astype(F32)
    spacing = jnp.sin((position + 0.5) * (math.pi / total_rows)) * (2.0 * total_rows / total_cols)
    gs[...] = 1.0 / (56.0 * spacing)
    for c in rims:
        c.wait()

    def send(src, dst, k, to_lat, to_lon):
        return pltpu.make_async_remote_copy(
            src_ref=src,
            dst_ref=dst,
            send_sem=sem_out.at[k],
            recv_sem=sem_got.at[k],
            device_id={"lat": to_lat, "lon": to_lon},
            device_id_type=pl.DeviceIdType.MESH,
        )

    south, north = [], []
    for k, (at, n) in enumerate(SPANS):
        tiles = pl.ds(1 + at, n)
        south.append(send(zc.at[tiles, pl.ds(192, 64)], hz.at[0, tiles], 6 + k, lat + 1, lon))
        north.append(send(zc.at[tiles, pl.ds(0, 64)], hz.at[1, tiles], 10 + k, lat - 1, lon))
    along = [send(packed.at[0], arrived.at[0], 0, lat, east), send(packed.at[1], arrived.at[1], 1, lat, west)]
    top, bottom = pl.ds(0, 32), pl.ds(96, 32)
    south_corners = [
        send(packed.at[0, bottom], corners.at[0, 0], 2, lat + 1, east),
        send(packed.at[1, bottom], corners.at[0, 1], 3, lat + 1, west),
    ]
    north_corners = [
        send(packed.at[0, top], corners.at[1, 0], 4, lat - 1, east),
        send(packed.at[1, top], corners.at[1, 1], 5, lat - 1, west),
    ]

    inside = jnp.logical_and(has_north, has_south)
    pl.semaphore_wait(barrier, jnp.where(inside, 8, 5))
    for k in range(len(SPANS)):
        for c, there in ((south[k], has_south), (north[k], has_north)):

            @pl.when(there)
            def _(c=c):
                c.start()

    for c in middle:
        c.wait()
    low = lax.broadcasted_iota(jnp.int32, (32, 128), 1) < 64
    for k in range(4):
        one, two, to = slice(64 * k, 64 * k + 32), slice(64 * k + 32, 64 * k + 64), slice(32 * k, 32 * k + 32)
        packed[0, to, :] = jnp.where(low, pltpu.roll(zc[TILES, one, :], 64, 1), zc[TILES, two, :])
        packed[1, to, :] = jnp.where(low, zc[1, one, :], pltpu.roll(zc[1, two, :], 64, 1))

    for j in (0, TILES + 1):
        zc[j] = jnp.zeros((ROWS, 128), F32)
    for k, s in enumerate(LAGS):
        m = pad_of(s)
        for ref in (ps[k], qs[k]):
            ref[:, 0:m, :] = jnp.zeros((TILES, m, 128), F32)
            ref[:, m + ROWS : m + ROWS + m, :] = jnp.zeros((TILES, m, 128), F32)
    clear(pt, qt)

    for c in along:
        c.start()

    @pl.when(has_south)
    def _():
        for c in south_corners:
            c.start()

    @pl.when(has_north)
    def _():
        for c in north_corners:
            c.start()

    def first(row):
        for j, d in differences(lambda j: zc[j, pl.ds(row, 8), :], TILES, LAGS):
            total = None
            for k, s in enumerate(LAGS):
                ps[k][j, pl.ds(row + pad_of(s), 8), :] = d[s][0]
                qs[k][j, pl.ds(row + pad_of(s), 8), :] = d[s][1]
                total = d[s][0] if total is None else total + d[s][0]
            cs[j, pl.ds(row, 8), :] = 2.0 * total

    def second(row, j):
        to_east = cs[j, pl.ds(row, 8), :]
        to_north = None
        for k, s in enumerate(LAGS):
            m = pad_of(s)
            above, below = pl.ds(row + (m - s), 8), pl.ds(row + (m + s), 8)
            to_east = to_east + (ps[k][j, above, :] + ps[k][j, below, :])
            diff = qs[k][j, above, :] - qs[k][j, below, :]
            to_north = diff if to_north is None else to_north + diff
        return to_east, to_north

    def put(rows, j, values):
        columns = slice(128 * j, 128 * j + 128)
        o_s[rows, columns] = values[0]
        o_f[0, rows, columns] = values[1]
        o_f[1, rows, columns] = values[2]
        o_h[rows, columns] = values[3]

    def keep_ends(row):
        for k, j in enumerate(ENDS):
            ends[k, 0, pl.ds(row, 8), :], ends[k, 1, pl.ds(row, 8), :] = second(row, j)

    def partial(row, side, to):
        for j in range(1, TILES - 1):
            en[side, 0, j, pl.ds(to, 8), :], en[side, 1, j, pl.ds(to, 8), :] = second(row, j)
        keep_ends(row)

    def finish(row):
        scale = gs[pl.ds(row, 8), :]
        for j in range(1, TILES - 1):
            put(pl.ds(row, 8), j, shade(*second(row, j), scale))
        keep_ends(row)

    def back(row, by):
        return pl.multiple_of(row - by, 8)

    def with_top(row):
        first(row)
        partial(back(row, 64), 0, back(row, 64))

    def with_middle(row):
        first(row)
        finish(back(row, 64))

    loop(0, 8, first)
    loop(8, 16, with_top)
    loop(16, 32, with_middle)
    loop(24, 32, lambda row: partial(row, 1, back(row, 192)))

    def clamp(side):
        row = 0 if side == 0 else ROWS - 1
        for j in range(1, TILES + 1):
            hz[side, j] = jnp.broadcast_to(zc[j, row : row + 1, :], (64, 128))

    @pl.when(jnp.logical_not(has_north))
    def _():
        clamp(0)

    @pl.when(jnp.logical_not(has_south))
    def _():
        clamp(1)

    for b, (at, n) in enumerate(BLOCKS):

        @pl.when(has_south)
        def _(b=b):
            north[b].wait_recv()

        @pl.when(has_north)
        def _(b=b):
            south[b].wait_recv()

        for side in range(2):
            halo_differences(
                side, lambda h, j, side=side, at=at: hz[side, at + j, 8 * h : 8 * h + 8, :], 0, n, pt, qt
            )
            for g in range(8):
                for j in range(n):
                    rows = slice(8 * g, 8 * g + 8)
                    sums = halo_sums(side, g, j, pt, qt, en[side, 0, at + j, rows, :], en[side, 1, at + j, rows, :])
                    rows = slice(8 * g + 192 * side, 8 * g + 192 * side + 8)
                    put(rows, at + j, shade(*sums, gs[rows, :]))

    for c in along:
        c.wait()

    @pl.when(has_south)
    def _():
        for c in north_corners:
            c.wait_recv()
        for c in south + south_corners:
            c.wait_send()

    @pl.when(has_north)
    def _():
        for c in south_corners:
            c.wait_recv()
        for c in north + north_corners:
            c.wait_send()


def store_kernel(
    i_s, i_f, i_h, hz, ends, gs, arrived, corners, o_s, o_f, o_h, hc, outer, pt, qt, stage, sem, sem_ends
):
    lat, n_lat = lax.axis_index("lat"), lax.axis_size("lat")

    def pieces(at):
        return (
            (i_s.at[at], o_s.at[at]),
            (i_f.at[(0, *at)], o_f.at[(0, *at)]),
            (i_f.at[(1, *at)], o_f.at[(1, *at)]),
            (i_h.at[at], o_h.at[at]),
        )

    copies = []
    for k in range(4):
        for n, (src, dst) in enumerate(pieces((pl.ds(64 * k, 64), pl.ds(128, COLS - 256)))):
            copies.append(pltpu.make_async_copy(src, dst, sem.at[n, k]))
    for c in copies:
        c.start()

    clear(pt, qt)
    for k, s in enumerate(LAGS):
        m = pad_of(s)
        outer[k][:, 0:m, :] = jnp.zeros((2, m, 128), F32)
        outer[k][:, m + ROWS : m + ROWS + m, :] = jnp.zeros((2, m, 128), F32)

    for side in range(2):
        pole = lat == (0 if side == 0 else n_lat - 1)

        @pl.when(jnp.logical_not(pole))
        def _(side=side):
            for e in range(2):
                both = corners[side, e]
                turned = pltpu.roll(both, 64, 1)
                hc[side, e, 0:32, :] = turned if e == 0 else both
                hc[side, e, 32:64, :] = both if e == 0 else turned

        @pl.when(pole)
        def _(side=side):
            for e in range(2):
                both = arrived[e, 0:8, :] if side == 0 else arrived[e, 120:128, :]
                turned = pltpu.roll(both, 64, 1)
                block = turned if (e == 0) == (side == 0) else both
                line = block[0:1] if side == 0 else block[7:8]
                hc[side, e] = jnp.broadcast_to(line, (64, 128))

    lane = lax.broadcasted_iota(jnp.int32, (8, 128), 1)

    def beyond(row):
        for r in range(8):
            half = 0 if r < 4 else 1
            at = pl.multiple_of(row * 4 + 8 * (r % 4), 8)
            to = pl.multiple_of(row * 8 + 8 * r, 8)
            for e in range(2):
                z = arrived[e, pl.ds(at, 8), :]
                for k, s in enumerate(LAGS):
                    by = (s + (64 if half == 0 else 0)) % 128 if e == 0 else (256 - s - (64 if half else 0)) % 128
                    turned = pltpu.roll(z, by, 1) if by else z
                    inside = lane < s if e == 0 else lane >= 128 - s
                    value = jnp.where(inside, turned * ((-1.0 if e == 0 else 1.0) / s), 0.0)
                    outer[k][e, pl.ds(to + pad_of(s), 8), :] = value

    loop(0, 4, beyond)

    for side in range(2):
        for e in range(2):

            def tiles(h, j, side=side, e=e):
                rows = slice(8 * h, 8 * h + 8)
                if e == 0:
                    return hc[side, 0, rows, :] if j == 0 else hz[side, j, rows, :]
                return hc[side, 1, rows, :] if j == 2 else hz[side, TILES - 1 + j, rows, :]

            halo_differences(side, tiles, e, 1, pt, qt)

    def sums(row, e):
        to_east = ends[e, 0, pl.ds(row, 8), :]
        to_north = ends[e, 1, pl.ds(row, 8), :]
        for k, s in enumerate(LAGS):
            m = pad_of(s)
            here = outer[k][e, pl.ds(row + m, 8), :]
            above = outer[k][e, pl.ds(row + (m - s), 8), :]
            below = outer[k][e, pl.ds(row + (m + s), 8), :]
            to_east = to_east + (above + below + 2.0 * here)
            diff = above - below
            to_north = to_north - diff if e == 0 else to_north + diff
        return to_east, to_north

    def put(row, e, values):
        for n, v in enumerate(values):
            stage[n, e, pl.ds(row, 8), :] = v

    def flush(k):
        for n in range(4):
            for e in range(2):
                at = (pl.ds(64 * k, 64), pl.ds(128 * ENDS[e], 128))
                dst = (o_s.at[at], o_f.at[(0, *at)], o_f.at[(1, *at)], o_h.at[at])[n]
                c = pltpu.make_async_copy(stage.at[n, e, pl.ds(64 * k, 64)], dst, sem_ends.at[n, e, k])
                c.start()
                copies.append(c)

    def middle(row):
        for r in range(4):
            here = pl.multiple_of(64 + row * 4 + 8 * r, 8)
            for e in range(2):
                put(here, e, shade(*sums(here, e), gs[pl.ds(here, 8), :]))

    loop(0, 4, middle)
    flush(1)
    flush(2)
    for side in range(2):
        for g in range(8):
            row = 8 * g + 192 * side
            for e in range(2):
                both = halo_sums(side, g, e, pt, qt, *sums(row, e))
                put(row, e, shade(*both, gs[row : row + 8, :]))
        flush(3 * side)
    for c in copies:
        c.wait()


OUTPUTS = ((ROWS, COLS), (2, ROWS, COLS), (ROWS, COLS))
BETWEEN = (
    (2, TILES + 2, HALO, 128),
    (2, 2, ROWS, 128),
    (ROWS, 128),
    (2, ROWS // 2, 128),
    (2, 2, HALO // 2, 128),
)


def local(x):
    anywhere = pl.BlockSpec(memory_space=pl.ANY)
    vmem = pl.BlockSpec(memory_space=pltpu.VMEM)
    columns = [pltpu.VMEM((TILES, ROWS + 2 * pad_of(s), 128), F32) for s in LAGS]

    def near(count):
        return [pltpu.VMEM((2, count, pad_of(s) if s >= 8 else 16, 128), F32) for s in LAGS]

    results = pl.pallas_call(
        exchange_kernel,
        out_shape=[pltpu.VMEM(shape, F32) for shape in OUTPUTS + BETWEEN],
        in_specs=[pl.BlockSpec(memory_space=pltpu.HBM)],
        out_specs=[vmem] * len(OUTPUTS + BETWEEN),
        scratch_shapes=[
            pltpu.VMEM((TILES + 2, ROWS, 128), F32),
            pltpu.VMEM((2, 128, 128), F32),
            columns,
            columns,
            pltpu.VMEM((TILES, ROWS, 128), F32),
            pltpu.VMEM((2, 2, TILES, HALO, 128), F32),
            near(MOST),
            near(MOST),
            pltpu.SemaphoreType.DMA((4, TILES)),
            pltpu.SemaphoreType.DMA((14,)),
            pltpu.SemaphoreType.DMA((14,)),
        ],
        compiler_params=pltpu.CompilerParams(collective_id=0, has_side_effects=True, vmem_limit_bytes=46 << 20),
        name="exchange",
    )(x)
    return tuple(
        pl.pallas_call(
            store_kernel,
            out_shape=[jax.ShapeDtypeStruct(shape, F32) for shape in OUTPUTS],
            in_specs=[vmem] * len(OUTPUTS + BETWEEN),
            out_specs=[anywhere] * 3,
            scratch_shapes=[
                pltpu.VMEM((2, 2, HALO, 128), F32),
                [pltpu.VMEM((2, ROWS + 2 * pad_of(s), 128), F32) for s in LAGS],
                near(2),
                near(2),
                pltpu.VMEM((4, 2, ROWS, 128), F32),
                pltpu.SemaphoreType.DMA((4, 4)),
                pltpu.SemaphoreType.DMA((4, 2, 4)),
            ],
            compiler_params=pltpu.CompilerParams(vmem_limit_bytes=16 << 20),
            name="store",
        )(*results)
    )


def solution(mesh):
    in_specs = (P("lat", "lon"),)
    out_specs = (P("lat", "lon"), P(None, "lat", "lon"), P("lat", "lon"))
    return jax.shard_map(local, mesh=mesh, in_specs=in_specs, out_specs=out_specs, check_vma=False)
```

```python
import math

import jax
import jax.numpy as jnp
from jax import lax
from jax.experimental import pallas as pl
from jax.experimental.pallas import tpu as pltpu
from jax.sharding import PartitionSpec as P

HALO = 64
LAGS = (1, 2, 4, 8, 16, 32, 64)
F32 = jnp.float32
ROWS, COLS, TILES = 256, 2048, 16


def pad_of(s):
    return max(8, s)


SMALLEST = 1.1754944e-38


def shade(east, north, east_scale):
    grad_east = east * east_scale
    grad_north = north * (1.0 / 56.0)
    squared = grad_east * grad_east + grad_north * grad_north
    inverse = lax.rsqrt(1.0 + squared)
    a = squared * lax.rsqrt(jnp.maximum(squared, SMALLEST)) * inverse
    b = 1.0 + inverse
    upper = a > 0.41421356 * b
    v = jnp.where(upper, a - b, a) / jnp.where(upper, a + b, b)
    z = v * v
    poly = ((2 * 8.05374449538e-2 * z - 2 * 1.38776856032e-1) * z + 2 * 1.99777106478e-1) * z - 2 * 3.33329491539e-1
    slope = (poly * z + 2.0) * v + jnp.where(upper, math.pi / 2, 0.0)
    down = -inverse
    facing_east = grad_east * down
    facing_north = grad_north * down
    shading = jnp.maximum((0.5 * (grad_east - grad_north) + math.sqrt(0.5)) * inverse, 0.0)
    return slope, facing_east, facing_north, shading


def differences(tiles, count, lags):
    lane = lax.broadcasted_iota(jnp.int32, (8, 128), 1)
    scaled, right, left = {}, {}, {}

    def at(j, s):
        if (j, s) not in scaled:
            if s == 0.5:
                scaled[j, s] = 2.0 * at(j, 1)
            elif s == 1:
                scaled[j, s] = tiles(j)
            else:
                scaled[j, s] = at(j, 1) * (1.0 / s)
        return scaled[j, s]

    def turned(j, s):
        if (j, s) not in right:
            right[j, s] = pltpu.roll(at(j, s), s, 1)
        return right[j, s]

    def turned_back(j, s):
        if s == 64:
            return turned(j, s)
        if (j, s) not in left:
            left[j, s] = pltpu.roll(at(j, s), 128 - s, 1)
        return left[j, s]

    for j in range(count):
        out = {}
        for s in lags:
            west = jnp.where(lane < s, turned(j, s), turned(j + 1, s))
            east = jnp.where(lane < 128 - s, turned_back(j + 1, s), turned_back(j + 2, s))
            out[s] = (east - west, east + west + at(j + 1, s / 2 if s > 1 else 0.5))
        yield j, out


BLOCKS = ((1, 4), (5, 4), (9, 4), (13, 2))
SPANS = ((0, 6), (6, 4), (10, 4), (14, 2))
MOST = 4
ENDS = (0, TILES - 1)


def clear(pt, qt):
    for k in range(3):
        for ref in (pt[k], qt[k]):
            zero = jnp.zeros((ref.shape[1], 8, 128), F32)
            ref[0, :, 8:16, :] = zero
            ref[1, :, 0:8, :] = zero


def halo_differences(side, tiles, at, count, pt, qt):
    for h in range(8):
        near = 7 - h if side == 0 else h
        lags = tuple(s for s in LAGS if pad_of(s) > 8 * near)
        for j, d in differences(lambda j, h=h: tiles(h, j), count, lags):
            for s in lags:
                if s < 8:
                    row = 0 if side == 0 else 8
                else:
                    row = 8 * h - (64 - s) if side == 0 else 8 * h
                k = LAGS.index(s)
                pt[k][side, at + j, row : row + 8, :] = d[s][0]
                qt[k][side, at + j, row : row + 8, :] = d[s][1]


def halo_sums(side, g, j, pt, qt, to_east, to_north):
    for k, s in enumerate(LAGS):
        if side == 0:
            if s < 8 and g == 0:
                row = 8 - s
            elif s >= 8 and 8 * g < s:
                row = 8 * g
            else:
                continue
            to_north = to_north + qt[k][0, j, row : row + 8, :]
        else:
            if s < 8 and g == 7:
                row = s
            elif s >= 8 and 8 * g + s >= 64:
                row = 8 * g + s - 64
            else:
                continue
            to_north = to_north - qt[k][1, j, row : row + 8, :]
        to_east = to_east + pt[k][side, j, row : row + 8, :]
    return to_east, to_north


def loop(lo, hi, body):
    def step(i, carry):
        body(pl.multiple_of(8 * i, 8))
        return carry

    lax.fori_loop(lo, hi, step, 0)


def exchange_kernel(
    x, o_s, o_f, o_h, hz, ends, gs, arrived, corners, zc, packed, ps, qs, cs, en, pt, qt, sem_in, sem_out, sem_got
):
    lat, lon = lax.axis_index("lat"), lax.axis_index("lon")
    n_lat, n_lon = lax.axis_size("lat"), lax.axis_size("lon")
    east, west = lax.rem(lon + 1, n_lon), lax.rem(lon + n_lon - 1, n_lon)
    has_north, has_south = lat > 0, lat < n_lat - 1

    def load(k, j, n):
        return pltpu.make_async_copy(
            x.at[pl.ds(64 * k, 64), pl.ds(128 * j, 128)], zc.at[j + 1, pl.ds(64 * k, 64)], sem_in.at[n]
        )

    def loaded(tiles, rows, n):
        pltpu.make_async_copy(zc.at[tiles, rows], zc.at[tiles, rows], sem_in.at[n]).wait()

    barrier = pltpu.get_barrier_semaphore()

    def greet(to_lat, to_lon):
        pl.semaphore_signal(
            barrier, inc=1, device_id={"lat": to_lat, "lon": to_lon}, device_id_type=pl.DeviceIdType.MESH
        )

    greet(lat, east)
    greet(lat, west)

    @pl.when(has_north)
    def _():
        for to in (lon, east, west):
            greet(lat - 1, to)

    @pl.when(has_south)
    def _():
        for to in (lon, east, west):
            greet(lat + 1, to)

    for n, (at, count) in enumerate(SPANS):
        for j in range(at, at + count):
            load(0, j, 2 * n).start()
            load(3, j, 2 * n + 1).start()
    for j in range(TILES):
        load(1, j, 2 * len(SPANS)).start()
        load(2, j, 2 * len(SPANS)).start()

    total_rows, total_cols = ROWS * n_lat, COLS * n_lon
    position = (lat * ROWS + lax.broadcasted_iota(jnp.int32, (ROWS, 128), 0)).astype(F32)
    spacing = jnp.sin((position + 0.5) * (math.pi / total_rows)) * (2.0 * total_rows / total_cols)
    gs[...] = 1.0 / (56.0 * spacing)

    def rim_loaded(n):
        at, count = SPANS[n]
        loaded(pl.ds(1 + at, count), pl.ds(0, 64), 2 * n)
        loaded(pl.ds(1 + at, count), pl.ds(192, 64), 2 * n + 1)

    def send(src, dst, group, k, to_lat, to_lon):
        return pltpu.make_async_remote_copy(
            src_ref=src,
            dst_ref=dst,
            send_sem=sem_out.at[group],
            recv_sem=sem_got.at[k],
            device_id={"lat": to_lat, "lon": to_lon},
            device_id_type=pl.DeviceIdType.MESH,
        )

    south, north = [], []
    for k, (at, n) in enumerate(SPANS):
        tiles = pl.ds(1 + at, n)
        south.append(send(zc.at[tiles, pl.ds(192, 64)], hz.at[0, tiles], 0, k, lat + 1, lon))
        north.append(send(zc.at[tiles, pl.ds(0, 64)], hz.at[1, tiles], 1, 4 + k, lat - 1, lon))
    along = [send(packed.at[0], arrived.at[0], 2, 8, lat, east), send(packed.at[1], arrived.at[1], 2, 8, lat, west)]
    top, bottom = pl.ds(0, 32), pl.ds(96, 32)
    south_corners = [
        send(packed.at[0, bottom], corners.at[0, 0], 3, 9, lat + 1, east),
        send(packed.at[1, bottom], corners.at[0, 1], 3, 9, lat + 1, west),
    ]
    north_corners = [
        send(packed.at[0, top], corners.at[1, 0], 4, 10, lat - 1, east),
        send(packed.at[1, top], corners.at[1, 1], 4, 10, lat - 1, west),
    ]

    all_tiles = pl.ds(1, TILES)
    all_south = send(zc.at[all_tiles, pl.ds(192, 64)], hz.at[0, all_tiles], 0, 0, lat + 1, lon)
    all_north = send(zc.at[all_tiles, pl.ds(0, 64)], hz.at[1, all_tiles], 1, 4, lat - 1, lon)
    all_along = send(packed, arrived, 2, 8, lat, east)
    all_south_corners = send(packed.at[:, bottom], corners.at[0], 3, 9, lat + 1, east)
    all_north_corners = send(packed.at[:, top], corners.at[1], 4, 10, lat - 1, east)
    inside = jnp.logical_and(has_north, has_south)
    pl.semaphore_wait(barrier, jnp.where(inside, 8, 5))
    rim_loaded(0)
    @pl.when(has_south)
    def _():
        for c in south[0:1]:
            c.start()

    @pl.when(has_north)
    def _():
        for c in north[0:1]:
            c.start()

    rim_loaded(1)
    @pl.when(has_south)
    def _():
        for c in south[1:2]:
            c.start()

    @pl.when(has_north)
    def _():
        for c in north[1:2]:
            c.start()

    rim_loaded(2)
    @pl.when(has_south)
    def _():
        for c in south[2:3]:
            c.start()

    @pl.when(has_north)
    def _():
        for c in north[2:3]:
            c.start()

    rim_loaded(3)
    @pl.when(has_south)
    def _():
        for c in south[3:4]:
            c.start()

    @pl.when(has_north)
    def _():
        for c in north[3:4]:
            c.start()

    loaded(pl.ds(1, TILES), pl.ds(64, 128), 2 * len(SPANS))
    low = lax.broadcasted_iota(jnp.int32, (32, 128), 1) < 64
    for k in range(4):
        one, two, to = slice(64 * k, 64 * k + 32), slice(64 * k + 32, 64 * k + 64), slice(32 * k, 32 * k + 32)
        packed[0, to, :] = jnp.where(low, pltpu.roll(zc[TILES, one, :], 64, 1), zc[TILES, two, :])
        packed[1, to, :] = jnp.where(low, zc[1, one, :], pltpu.roll(zc[1, two, :], 64, 1))

    odd = lax.rem(lon, 2) == 1

    @pl.when(jnp.logical_not(odd))
    def _():
        along[1].start()

    @pl.when(odd)
    def _():
        along[0].start()

    @pl.when(has_south)
    def _():
        for c in south_corners:
            c.start()

    @pl.when(has_north)
    def _():
        for c in north_corners:
            c.start()

    for j in (0, TILES + 1):
        zc[j] = jnp.zeros((ROWS, 128), F32)
    for k, s in enumerate(LAGS):
        m = pad_of(s)
        for ref in (ps[k], qs[k]):
            ref[:, 0:m, :] = jnp.zeros((TILES, m, 128), F32)
            ref[:, m + ROWS : m + ROWS + m, :] = jnp.zeros((TILES, m, 128), F32)
    clear(pt, qt)

    @pl.when(odd)
    def _():
        along[1].start()

    @pl.when(jnp.logical_not(odd))
    def _():
        along[0].start()

    def first(row):
        for j, d in differences(lambda j: zc[j, pl.ds(row, 8), :], TILES, LAGS):
            total = None
            for k, s in enumerate(LAGS):
                ps[k][j, pl.ds(row + pad_of(s), 8), :] = d[s][0]
                qs[k][j, pl.ds(row + pad_of(s), 8), :] = d[s][1]
                total = d[s][0] if total is None else total + d[s][0]
            cs[j, pl.ds(row, 8), :] = 2.0 * total

    def second(row, j):
        to_east = cs[j, pl.ds(row, 8), :]
        to_north = None
        for k, s in enumerate(LAGS):
            m = pad_of(s)
            above, below = pl.ds(row + (m - s), 8), pl.ds(row + (m + s), 8)
            to_east = to_east + (ps[k][j, above, :] + ps[k][j, below, :])
            diff = qs[k][j, above, :] - qs[k][j, below, :]
            to_north = diff if to_north is None else to_north + diff
        return to_east, to_north

    def put(rows, j, values):
        columns = slice(128 * j, 128 * j + 128)
        o_s[rows, columns] = values[0]
        o_f[0, rows, columns] = values[1]
        o_f[1, rows, columns] = values[2]
        o_h[rows, columns] = values[3]

    def keep_ends(row):
        for k, j in enumerate(ENDS):
            ends[k, 0, pl.ds(row, 8), :], ends[k, 1, pl.ds(row, 8), :] = second(row, j)

    def partial(row, side, to):
        for j in range(1, TILES - 1):
            en[side, 0, j, pl.ds(to, 8), :], en[side, 1, j, pl.ds(to, 8), :] = second(row, j)
        keep_ends(row)

    def finish(row):
        scale = gs[pl.ds(row, 8), :]
        for j in range(1, TILES - 1):
            put(pl.ds(row, 8), j, shade(*second(row, j), scale))
        keep_ends(row)

    def back(row, by):
        return pl.multiple_of(row - by, 8)

    def with_top(row):
        first(row)
        partial(back(row, 64), 0, back(row, 64))

    def with_middle(row):
        first(row)
        finish(back(row, 64))

    loop(0, 8, first)
    loop(8, 16, with_top)
    loop(16, 32, with_middle)
    loop(24, 32, lambda row: partial(row, 1, back(row, 192)))

    def clamp(side):
        row = 0 if side == 0 else ROWS - 1
        for j in range(1, TILES + 1):
            hz[side, j] = jnp.broadcast_to(zc[j, row : row + 1, :], (64, 128))

    @pl.when(jnp.logical_not(has_north))
    def _():
        clamp(0)

    @pl.when(jnp.logical_not(has_south))
    def _():
        clamp(1)

    for b, (at, n) in enumerate(BLOCKS):

        @pl.when(has_south)
        def _(b=b):
            north[b].wait_recv()

        @pl.when(has_north)
        def _(b=b):
            south[b].wait_recv()

        for side in range(2):
            halo_differences(
                side, lambda h, j, side=side, at=at: hz[side, at + j, 8 * h : 8 * h + 8, :], 0, n, pt, qt
            )
            for g in range(8):
                for j in range(n):
                    rows = slice(8 * g, 8 * g + 8)
                    sums = halo_sums(side, g, j, pt, qt, en[side, 0, at + j, rows, :], en[side, 1, at + j, rows, :])
                    rows = slice(8 * g + 192 * side, 8 * g + 192 * side + 8)
                    put(rows, at + j, shade(*sums, gs[rows, :]))

    all_along.wait()

    @pl.when(has_south)
    def _():
        all_north_corners.wait_recv()
        all_south.wait_send()
        all_south_corners.wait_send()

    @pl.when(has_north)
    def _():
        all_south_corners.wait_recv()
        all_north.wait_send()
        all_north_corners.wait_send()


def store_kernel(
    i_s, i_f, i_h, hz, ends, gs, arrived, corners, o_s, o_f, o_h, hc, outer, pt, qt, stage, sem
):
    lat, n_lat = lax.axis_index("lat"), lax.axis_size("lat")

    def pieces(at):
        return (
            (i_s.at[at], o_s.at[at]),
            (i_f.at[(0, *at)], o_f.at[(0, *at)]),
            (i_f.at[(1, *at)], o_f.at[(1, *at)]),
            (i_h.at[at], o_h.at[at]),
        )

    of = (0, 1, 1, 2)
    for k in range(4):
        for n, (src, dst) in enumerate(pieces((pl.ds(64 * k, 64), pl.ds(128, COLS - 256)))):
            pltpu.make_async_copy(src, dst, sem.at[of[n]]).start()

    clear(pt, qt)
    for k, s in enumerate(LAGS):
        m = pad_of(s)
        outer[k][:, 0:m, :] = jnp.zeros((2, m, 128), F32)
        outer[k][:, m + ROWS : m + ROWS + m, :] = jnp.zeros((2, m, 128), F32)

    for side in range(2):
        pole = lat == (0 if side == 0 else n_lat - 1)

        @pl.when(jnp.logical_not(pole))
        def _(side=side):
            for e in range(2):
                both = corners[side, e]
                turned = pltpu.roll(both, 64, 1)
                hc[side, e, 0:32, :] = turned if e == 0 else both
                hc[side, e, 32:64, :] = both if e == 0 else turned

        @pl.when(pole)
        def _(side=side):
            for e in range(2):
                both = arrived[e, 0:8, :] if side == 0 else arrived[e, 120:128, :]
                turned = pltpu.roll(both, 64, 1)
                block = turned if (e == 0) == (side == 0) else both
                line = block[0:1] if side == 0 else block[7:8]
                hc[side, e] = jnp.broadcast_to(line, (64, 128))

    lane = lax.broadcasted_iota(jnp.int32, (8, 128), 1)

    def beyond(row):
        for r in range(8):
            half = 0 if r < 4 else 1
            at = pl.multiple_of(row * 4 + 8 * (r % 4), 8)
            to = pl.multiple_of(row * 8 + 8 * r, 8)
            for e in range(2):
                z = arrived[e, pl.ds(at, 8), :]
                for k, s in enumerate(LAGS):
                    by = (s + (64 if half == 0 else 0)) % 128 if e == 0 else (256 - s - (64 if half else 0)) % 128
                    turned = pltpu.roll(z, by, 1) if by else z
                    inside = lane < s if e == 0 else lane >= 128 - s
                    value = jnp.where(inside, turned * ((-1.0 if e == 0 else 1.0) / s), 0.0)
                    outer[k][e, pl.ds(to + pad_of(s), 8), :] = value

    loop(0, 4, beyond)

    for side in range(2):
        for e in range(2):

            def tiles(h, j, side=side, e=e):
                rows = slice(8 * h, 8 * h + 8)
                if e == 0:
                    return hc[side, 0, rows, :] if j == 0 else hz[side, j, rows, :]
                return hc[side, 1, rows, :] if j == 2 else hz[side, TILES - 1 + j, rows, :]

            halo_differences(side, tiles, e, 1, pt, qt)

    def sums(row, e):
        to_east = ends[e, 0, pl.ds(row, 8), :]
        to_north = ends[e, 1, pl.ds(row, 8), :]
        for k, s in enumerate(LAGS):
            m = pad_of(s)
            here = outer[k][e, pl.ds(row + m, 8), :]
            above = outer[k][e, pl.ds(row + (m - s), 8), :]
            below = outer[k][e, pl.ds(row + (m + s), 8), :]
            to_east = to_east + (above + below + 2.0 * here)
            diff = above - below
            to_north = to_north - diff if e == 0 else to_north + diff
        return to_east, to_north

    def put(row, e, values):
        for n, v in enumerate(values):
            stage[n, e, pl.ds(row, 8), :] = v

    def flush(k):
        for n in range(4):
            for e in range(2):
                at = (pl.ds(64 * k, 64), pl.ds(128 * ENDS[e], 128))
                dst = (o_s.at[at], o_f.at[(0, *at)], o_f.at[(1, *at)], o_h.at[at])[n]
                pltpu.make_async_copy(stage.at[n, e, pl.ds(64 * k, 64)], dst, sem.at[of[n]]).start()

    def middle(row):
        for r in range(4):
            here = pl.multiple_of(64 + row * 4 + 8 * r, 8)
            for e in range(2):
                put(here, e, shade(*sums(here, e), gs[pl.ds(here, 8), :]))

    loop(0, 4, middle)
    flush(1)
    flush(2)
    for side in range(2):
        for g in range(8):
            row = 8 * g + 192 * side
            for e in range(2):
                both = halo_sums(side, g, e, pt, qt, *sums(row, e))
                put(row, e, shade(*both, gs[row : row + 8, :]))
        flush(3 * side)
    for n, (src, dst) in enumerate(((i_s, o_s), (i_f, o_f), (i_h, o_h))):
        pltpu.make_async_copy(src, dst, sem.at[n]).wait()


OUTPUTS = ((ROWS, COLS), (2, ROWS, COLS), (ROWS, COLS))
BETWEEN = (
    (2, TILES + 2, HALO, 128),
    (2, 2, ROWS, 128),
    (ROWS, 128),
    (2, ROWS // 2, 128),
    (2, 2, HALO // 2, 128),
)


def local(x):
    anywhere = pl.BlockSpec(memory_space=pl.ANY)
    vmem = pl.BlockSpec(memory_space=pltpu.VMEM)
    columns = [pltpu.VMEM((TILES, ROWS + 2 * pad_of(s), 128), F32) for s in LAGS]

    def near(count):
        return [pltpu.VMEM((2, count, pad_of(s) if s >= 8 else 16, 128), F32) for s in LAGS]

    results = pl.pallas_call(
        exchange_kernel,
        out_shape=[pltpu.VMEM(shape, F32) for shape in OUTPUTS + BETWEEN],
        in_specs=[pl.BlockSpec(memory_space=pltpu.HBM)],
        out_specs=[vmem] * len(OUTPUTS + BETWEEN),
        scratch_shapes=[
            pltpu.VMEM((TILES + 2, ROWS, 128), F32),
            pltpu.VMEM((2, 128, 128), F32),
            columns,
            columns,
            pltpu.VMEM((TILES, ROWS, 128), F32),
            pltpu.VMEM((2, 2, TILES, HALO, 128), F32),
            near(MOST),
            near(MOST),
            pltpu.SemaphoreType.DMA((2 * len(SPANS) + 1,)),
            pltpu.SemaphoreType.DMA((5,)),
            pltpu.SemaphoreType.DMA((11,)),
        ],
        compiler_params=pltpu.CompilerParams(collective_id=0, has_side_effects=True, vmem_limit_bytes=46 << 20),
        name="exchange",
    )(x)
    return tuple(
        pl.pallas_call(
            store_kernel,
            out_shape=[jax.ShapeDtypeStruct(shape, F32) for shape in OUTPUTS],
            in_specs=[vmem] * len(OUTPUTS + BETWEEN),
            out_specs=[anywhere] * 3,
            scratch_shapes=[
                pltpu.VMEM((2, 2, HALO, 128), F32),
                [pltpu.VMEM((2, ROWS + 2 * pad_of(s), 128), F32) for s in LAGS],
                near(2),
                near(2),
                pltpu.VMEM((4, 2, ROWS, 128), F32),
                pltpu.SemaphoreType.DMA((3,)),
            ],
            compiler_params=pltpu.CompilerParams(vmem_limit_bytes=16 << 20),
            name="store",
        )(*results)
    )


def solution(mesh):
    in_specs = (P("lat", "lon"),)
    out_specs = (P("lat", "lon"), P(None, "lat", "lon"), P("lat", "lon"))
    return jax.shard_map(local, mesh=mesh, in_specs=in_specs, out_specs=out_specs, check_vma=False)
```

```python
import math

import jax
import jax.numpy as jnp
from jax import lax
from jax.experimental import pallas as pl
from jax.experimental.pallas import tpu as pltpu
from jax.sharding import PartitionSpec as P

HALO = 64
LAGS = (1, 2, 4, 8, 16, 32, 64)
F32 = jnp.float32
ROWS, COLS, TILES = 256, 2048, 16


def pad_of(s):
    return max(8, s)


SMALLEST = 1.1754944e-38


def shade(east, north, east_scale):
    grad_east = east * east_scale
    grad_north = north * (1.0 / 56.0)
    squared = grad_east * grad_east + grad_north * grad_north
    inverse = lax.rsqrt(1.0 + squared)
    a = squared * lax.rsqrt(jnp.maximum(squared, SMALLEST)) * inverse
    b = 1.0 + inverse
    upper = a > 0.41421356 * b
    v = jnp.where(upper, a - b, a) / jnp.where(upper, a + b, b)
    z = v * v
    poly = ((2 * 8.05374449538e-2 * z - 2 * 1.38776856032e-1) * z + 2 * 1.99777106478e-1) * z - 2 * 3.33329491539e-1
    slope = (poly * z + 2.0) * v + jnp.where(upper, math.pi / 2, 0.0)
    down = -inverse
    facing_east = grad_east * down
    facing_north = grad_north * down
    shading = jnp.maximum((0.5 * (grad_east - grad_north) + math.sqrt(0.5)) * inverse, 0.0)
    return slope, facing_east, facing_north, shading


def differences(tiles, count, lags):
    lane = lax.broadcasted_iota(jnp.int32, (8, 128), 1)
    scaled, right, left = {}, {}, {}

    def at(j, s):
        if (j, s) not in scaled:
            if s == 0.5:
                scaled[j, s] = 2.0 * at(j, 1)
            elif s == 1:
                scaled[j, s] = tiles(j)
            else:
                scaled[j, s] = at(j, 1) * (1.0 / s)
        return scaled[j, s]

    def turned(j, s):
        if (j, s) not in right:
            right[j, s] = pltpu.roll(at(j, s), s, 1)
        return right[j, s]

    def turned_back(j, s):
        if s == 64:
            return turned(j, s)
        if (j, s) not in left:
            left[j, s] = pltpu.roll(at(j, s), 128 - s, 1)
        return left[j, s]

    for j in range(count):
        out = {}
        for s in lags:
            west = jnp.where(lane < s, turned(j, s), turned(j + 1, s))
            east = jnp.where(lane < 128 - s, turned_back(j + 1, s), turned_back(j + 2, s))
            out[s] = (east - west, east + west + at(j + 1, s / 2 if s > 1 else 0.5))
        yield j, out


BLOCKS = ((1, 4), (5, 4), (9, 4), (13, 2))
SPANS = ((0, 6), (6, 4), (10, 4), (14, 2))
MOST = 4
ENDS = (0, TILES - 1)


def clear(pt, qt):
    for k in range(3):
        for ref in (pt[k], qt[k]):
            zero = jnp.zeros((ref.shape[1], 8, 128), F32)
            ref[0, :, 8:16, :] = zero
            ref[1, :, 0:8, :] = zero


def halo_differences(side, tiles, at, count, pt, qt):
    for h in range(8):
        near = 7 - h if side == 0 else h
        lags = tuple(s for s in LAGS if pad_of(s) > 8 * near)
        for j, d in differences(lambda j, h=h: tiles(h, j), count, lags):
            for s in lags:
                if s < 8:
                    row = 0 if side == 0 else 8
                else:
                    row = 8 * h - (64 - s) if side == 0 else 8 * h
                k = LAGS.index(s)
                pt[k][side, at + j, row : row + 8, :] = d[s][0]
                qt[k][side, at + j, row : row + 8, :] = d[s][1]


def halo_sums(side, g, j, pt, qt, to_east, to_north):
    for k, s in enumerate(LAGS):
        if side == 0:
            if s < 8 and g == 0:
                row = 8 - s
            elif s >= 8 and 8 * g < s:
                row = 8 * g
            else:
                continue
            to_north = to_north + qt[k][0, j, row : row + 8, :]
        else:
            if s < 8 and g == 7:
                row = s
            elif s >= 8 and 8 * g + s >= 64:
                row = 8 * g + s - 64
            else:
                continue
            to_north = to_north - qt[k][1, j, row : row + 8, :]
        to_east = to_east + pt[k][side, j, row : row + 8, :]
    return to_east, to_north


def loop(lo, hi, body):
    def step(i, carry):
        body(pl.multiple_of(8 * i, 8))
        return carry

    lax.fori_loop(lo, hi, step, 0)


def exchange_kernel(
    x, o_s, o_f, o_h, hz, ends, gs, arrived, corners, zc, packed, ps, qs, cs, en, pt, qt, sem_in, sem_out, sem_got
):
    lat, lon = lax.axis_index("lat"), lax.axis_index("lon")
    n_lat, n_lon = lax.axis_size("lat"), lax.axis_size("lon")
    east, west = lax.rem(lon + 1, n_lon), lax.rem(lon + n_lon - 1, n_lon)
    has_north, has_south = lat > 0, lat < n_lat - 1

    def load(k, j, n):
        return pltpu.make_async_copy(
            x.at[pl.ds(64 * k, 64), pl.ds(128 * j, 128)], zc.at[j + 1, pl.ds(64 * k, 64)], sem_in.at[n]
        )

    def loaded(tiles, rows, n):
        pltpu.make_async_copy(zc.at[tiles, rows], zc.at[tiles, rows], sem_in.at[n]).wait()

    barrier = pltpu.get_barrier_semaphore()

    def greet(to_lat, to_lon):
        pl.semaphore_signal(
            barrier, inc=1, device_id={"lat": to_lat, "lon": to_lon}, device_id_type=pl.DeviceIdType.MESH
        )

    greet(lat, east)
    greet(lat, west)

    @pl.when(has_north)
    def _():
        for to in (lon, east, west):
            greet(lat - 1, to)

    @pl.when(has_south)
    def _():
        for to in (lon, east, west):
            greet(lat + 1, to)

    for n, (at, count) in enumerate(SPANS):
        for j in range(at, at + count):
            load(0, j, 2 * n).start()
            load(3, j, 2 * n + 1).start()
    for j in range(TILES):
        load(1, j, 2 * len(SPANS)).start()
        load(2, j, 2 * len(SPANS)).start()

    total_rows, total_cols = ROWS * n_lat, COLS * n_lon
    position = (lat * ROWS + lax.broadcasted_iota(jnp.int32, (ROWS, 128), 0)).astype(F32)
    spacing = jnp.sin((position + 0.5) * (math.pi / total_rows)) * (2.0 * total_rows / total_cols)
    gs[...] = 1.0 / (56.0 * spacing)

    def rim_loaded(n):
        at, count = SPANS[n]
        loaded(pl.ds(1 + at, count), pl.ds(0, 64), 2 * n)
        loaded(pl.ds(1 + at, count), pl.ds(192, 64), 2 * n + 1)

    def send(src, dst, group, k, to_lat, to_lon):
        return pltpu.make_async_remote_copy(
            src_ref=src,
            dst_ref=dst,
            send_sem=sem_out.at[group],
            recv_sem=sem_got.at[k],
            device_id={"lat": to_lat, "lon": to_lon},
            device_id_type=pl.DeviceIdType.MESH,
        )

    south, north = [], []
    for k, (at, n) in enumerate(SPANS):
        tiles = pl.ds(1 + at, n)
        south.append(send(zc.at[tiles, pl.ds(192, 64)], hz.at[0, tiles], 0, k, lat + 1, lon))
        north.append(send(zc.at[tiles, pl.ds(0, 64)], hz.at[1, tiles], 1, 4 + k, lat - 1, lon))
    along = [send(packed.at[0], arrived.at[0], 2, 8, lat, east), send(packed.at[1], arrived.at[1], 2, 8, lat, west)]
    top, bottom = pl.ds(0, 32), pl.ds(96, 32)
    south_corners = [
        send(packed.at[0, bottom], corners.at[0, 0], 3, 9, lat + 1, east),
        send(packed.at[1, bottom], corners.at[0, 1], 3, 9, lat + 1, west),
    ]
    north_corners = [
        send(packed.at[0, top], corners.at[1, 0], 4, 10, lat - 1, east),
        send(packed.at[1, top], corners.at[1, 1], 4, 10, lat - 1, west),
    ]

    all_tiles = pl.ds(1, TILES)
    all_south = send(zc.at[all_tiles, pl.ds(192, 64)], hz.at[0, all_tiles], 0, 0, lat + 1, lon)
    all_north = send(zc.at[all_tiles, pl.ds(0, 64)], hz.at[1, all_tiles], 1, 4, lat - 1, lon)
    all_along = send(packed, arrived, 2, 8, lat, east)
    all_south_corners = send(packed.at[:, bottom], corners.at[0], 3, 9, lat + 1, east)
    all_north_corners = send(packed.at[:, top], corners.at[1], 4, 10, lat - 1, east)
    inside = jnp.logical_and(has_north, has_south)
    rim_loaded(0)
    rim_loaded(1)
    rim_loaded(2)
    rim_loaded(3)
    loaded(pl.ds(1, TILES), pl.ds(64, 128), 2 * len(SPANS))
    low = lax.broadcasted_iota(jnp.int32, (32, 128), 1) < 64
    for k in range(4):
        one, two, to = slice(64 * k, 64 * k + 32), slice(64 * k + 32, 64 * k + 64), slice(32 * k, 32 * k + 32)
        packed[0, to, :] = jnp.where(low, pltpu.roll(zc[TILES, one, :], 64, 1), zc[TILES, two, :])
        packed[1, to, :] = jnp.where(low, zc[1, one, :], pltpu.roll(zc[1, two, :], 64, 1))

    pl.semaphore_wait(barrier, jnp.where(inside, 8, 5))
    odd = lax.rem(lon, 2) == 1

    def start_rest(now):
        def begin(when, *group):
            @pl.when(jnp.logical_and(now, when))
            def _():
                for c in group:
                    c.start()

        begin(jnp.logical_not(odd), along[1])
        begin(odd, along[0])
        begin(has_south, *south_corners)
        begin(has_north, *north_corners)
        begin(odd, along[1])
        begin(jnp.logical_not(odd), along[0])

    quarter = lax.rem(lat, 4)
    level = jnp.logical_or(quarter == 1, quarter == 2)
    start_rest(jnp.logical_not(level))
    @pl.when(has_south)
    def _():
        for c in south[0:1]:
            c.start()

    @pl.when(has_north)
    def _():
        for c in north[0:1]:
            c.start()

    @pl.when(has_south)
    def _():
        for c in south[1:2]:
            c.start()

    @pl.when(has_north)
    def _():
        for c in north[1:2]:
            c.start()

    @pl.when(has_south)
    def _():
        for c in south[2:3]:
            c.start()

    @pl.when(has_north)
    def _():
        for c in north[2:3]:
            c.start()

    @pl.when(has_south)
    def _():
        for c in south[3:4]:
            c.start()

    @pl.when(has_north)
    def _():
        for c in north[3:4]:
            c.start()

    for j in (0, TILES + 1):
        zc[j] = jnp.zeros((ROWS, 128), F32)
    for k, s in enumerate(LAGS):
        m = pad_of(s)
        for ref in (ps[k], qs[k]):
            ref[:, 0:m, :] = jnp.zeros((TILES, m, 128), F32)
            ref[:, m + ROWS : m + ROWS + m, :] = jnp.zeros((TILES, m, 128), F32)
    clear(pt, qt)

    start_rest(level)

    def first(row):
        for j, d in differences(lambda j: zc[j, pl.ds(row, 8), :], TILES, LAGS):
            total = None
            for k, s in enumerate(LAGS):
                ps[k][j, pl.ds(row + pad_of(s), 8), :] = d[s][0]
                qs[k][j, pl.ds(row + pad_of(s), 8), :] = d[s][1]
                total = d[s][0] if total is None else total + d[s][0]
            cs[j, pl.ds(row, 8), :] = 2.0 * total

    def second(row, j):
        to_east = cs[j, pl.ds(row, 8), :]
        to_north = None
        for k, s in enumerate(LAGS):
            m = pad_of(s)
            above, below = pl.ds(row + (m - s), 8), pl.ds(row + (m + s), 8)
            to_east = to_east + (ps[k][j, above, :] + ps[k][j, below, :])
            diff = qs[k][j, above, :] - qs[k][j, below, :]
            to_north = diff if to_north is None else to_north + diff
        return to_east, to_north

    def put(rows, j, values):
        columns = slice(128 * j, 128 * j + 128)
        o_s[rows, columns] = values[0]
        o_f[0, rows, columns] = values[1]
        o_f[1, rows, columns] = values[2]
        o_h[rows, columns] = values[3]

    def keep_ends(row):
        for k, j in enumerate(ENDS):
            ends[k, 0, pl.ds(row, 8), :], ends[k, 1, pl.ds(row, 8), :] = second(row, j)

    def partial(row, side, to):
        for j in range(1, TILES - 1):
            en[side, 0, j, pl.ds(to, 8), :], en[side, 1, j, pl.ds(to, 8), :] = second(row, j)
        keep_ends(row)

    def finish(row):
        scale = gs[pl.ds(row, 8), :]
        for j in range(1, TILES - 1):
            put(pl.ds(row, 8), j, shade(*second(row, j), scale))
        keep_ends(row)

    def back(row, by):
        return pl.multiple_of(row - by, 8)

    def with_top(row):
        first(row)
        partial(back(row, 64), 0, back(row, 64))

    def with_middle(row):
        first(row)
        finish(back(row, 64))

    loop(0, 8, first)
    loop(8, 16, with_top)
    loop(16, 32, with_middle)
    loop(24, 32, lambda row: partial(row, 1, back(row, 192)))

    def clamp(side):
        row = 0 if side == 0 else ROWS - 1
        for j in range(1, TILES + 1):
            hz[side, j] = jnp.broadcast_to(zc[j, row : row + 1, :], (64, 128))

    @pl.when(jnp.logical_not(has_north))
    def _():
        clamp(0)

    @pl.when(jnp.logical_not(has_south))
    def _():
        clamp(1)

    for b, (at, n) in enumerate(BLOCKS):

        @pl.when(has_south)
        def _(b=b):
            north[b].wait_recv()

        @pl.when(has_north)
        def _(b=b):
            south[b].wait_recv()

        for side in range(2):
            halo_differences(
                side, lambda h, j, side=side, at=at: hz[side, at + j, 8 * h : 8 * h + 8, :], 0, n, pt, qt
            )
            for g in range(8):
                for j in range(n):
                    rows = slice(8 * g, 8 * g + 8)
                    sums = halo_sums(side, g, j, pt, qt, en[side, 0, at + j, rows, :], en[side, 1, at + j, rows, :])
                    rows = slice(8 * g + 192 * side, 8 * g + 192 * side + 8)
                    put(rows, at + j, shade(*sums, gs[rows, :]))

    all_along.wait()

    @pl.when(has_south)
    def _():
        all_north_corners.wait_recv()
        all_south.wait_send()
        all_south_corners.wait_send()

    @pl.when(has_north)
    def _():
        all_south_corners.wait_recv()
        all_north.wait_send()
        all_north_corners.wait_send()


def store_kernel(
    i_s, i_f, i_h, hz, ends, gs, arrived, corners, o_s, o_f, o_h, hc, outer, pt, qt, stage, sem
):
    lat, n_lat = lax.axis_index("lat"), lax.axis_size("lat")

    def pieces(at):
        return (
            (i_s.at[at], o_s.at[at]),
            (i_f.at[(0, *at)], o_f.at[(0, *at)]),
            (i_f.at[(1, *at)], o_f.at[(1, *at)]),
            (i_h.at[at], o_h.at[at]),
        )

    of = (0, 1, 1, 2)
    for k in range(4):
        for n, (src, dst) in enumerate(pieces((pl.ds(64 * k, 64), pl.ds(128, COLS - 256)))):
            pltpu.make_async_copy(src, dst, sem.at[of[n]]).start()

    clear(pt, qt)
    for k, s in enumerate(LAGS):
        m = pad_of(s)
        outer[k][:, 0:m, :] = jnp.zeros((2, m, 128), F32)
        outer[k][:, m + ROWS : m + ROWS + m, :] = jnp.zeros((2, m, 128), F32)

    for side in range(2):
        pole = lat == (0 if side == 0 else n_lat - 1)

        @pl.when(jnp.logical_not(pole))
        def _(side=side):
            for e in range(2):
                both = corners[side, e]
                turned = pltpu.roll(both, 64, 1)
                hc[side, e, 0:32, :] = turned if e == 0 else both
                hc[side, e, 32:64, :] = both if e == 0 else turned

        @pl.when(pole)
        def _(side=side):
            for e in range(2):
                both = arrived[e, 0:8, :] if side == 0 else arrived[e, 120:128, :]
                turned = pltpu.roll(both, 64, 1)
                block = turned if (e == 0) == (side == 0) else both
                line = block[0:1] if side == 0 else block[7:8]
                hc[side, e] = jnp.broadcast_to(line, (64, 128))

    lane = lax.broadcasted_iota(jnp.int32, (8, 128), 1)

    def beyond(row):
        for r in range(8):
            half = 0 if r < 4 else 1
            at = pl.multiple_of(row * 4 + 8 * (r % 4), 8)
            to = pl.multiple_of(row * 8 + 8 * r, 8)
            for e in range(2):
                z = arrived[e, pl.ds(at, 8), :]
                for k, s in enumerate(LAGS):
                    by = (s + (64 if half == 0 else 0)) % 128 if e == 0 else (256 - s - (64 if half else 0)) % 128
                    turned = pltpu.roll(z, by, 1) if by else z
                    inside = lane < s if e == 0 else lane >= 128 - s
                    value = jnp.where(inside, turned * ((-1.0 if e == 0 else 1.0) / s), 0.0)
                    outer[k][e, pl.ds(to + pad_of(s), 8), :] = value

    loop(0, 4, beyond)

    for side in range(2):
        for e in range(2):

            def tiles(h, j, side=side, e=e):
                rows = slice(8 * h, 8 * h + 8)
                if e == 0:
                    return hc[side, 0, rows, :] if j == 0 else hz[side, j, rows, :]
                return hc[side, 1, rows, :] if j == 2 else hz[side, TILES - 1 + j, rows, :]

            halo_differences(side, tiles, e, 1, pt, qt)

    def sums(row, e):
        to_east = ends[e, 0, pl.ds(row, 8), :]
        to_north = ends[e, 1, pl.ds(row, 8), :]
        for k, s in enumerate(LAGS):
            m = pad_of(s)
            here = outer[k][e, pl.ds(row + m, 8), :]
            above = outer[k][e, pl.ds(row + (m - s), 8), :]
            below = outer[k][e, pl.ds(row + (m + s), 8), :]
            to_east = to_east + (above + below + 2.0 * here)
            diff = above - below
            to_north = to_north - diff if e == 0 else to_north + diff
        return to_east, to_north

    def put(row, e, values):
        for n, v in enumerate(values):
            stage[n, e, pl.ds(row, 8), :] = v

    def flush(k):
        for n in range(4):
            for e in range(2):
                at = (pl.ds(64 * k, 64), pl.ds(128 * ENDS[e], 128))
                dst = (o_s.at[at], o_f.at[(0, *at)], o_f.at[(1, *at)], o_h.at[at])[n]
                pltpu.make_async_copy(stage.at[n, e, pl.ds(64 * k, 64)], dst, sem.at[of[n]]).start()

    def middle(row):
        for r in range(4):
            here = pl.multiple_of(64 + row * 4 + 8 * r, 8)
            for e in range(2):
                put(here, e, shade(*sums(here, e), gs[pl.ds(here, 8), :]))

    loop(0, 4, middle)
    flush(1)
    flush(2)
    for side in range(2):
        for g in range(8):
            row = 8 * g + 192 * side
            for e in range(2):
                both = halo_sums(side, g, e, pt, qt, *sums(row, e))
                put(row, e, shade(*both, gs[row : row + 8, :]))
        flush(3 * side)
    for n, (src, dst) in enumerate(((i_s, o_s), (i_f, o_f), (i_h, o_h))):
        pltpu.make_async_copy(src, dst, sem.at[n]).wait()


OUTPUTS = ((ROWS, COLS), (2, ROWS, COLS), (ROWS, COLS))
BETWEEN = (
    (2, TILES + 2, HALO, 128),
    (2, 2, ROWS, 128),
    (ROWS, 128),
    (2, ROWS // 2, 128),
    (2, 2, HALO // 2, 128),
)


def local(x):
    anywhere = pl.BlockSpec(memory_space=pl.ANY)
    vmem = pl.BlockSpec(memory_space=pltpu.VMEM)
    columns = [pltpu.VMEM((TILES, ROWS + 2 * pad_of(s), 128), F32) for s in LAGS]

    def near(count):
        return [pltpu.VMEM((2, count, pad_of(s) if s >= 8 else 16, 128), F32) for s in LAGS]

    results = pl.pallas_call(
        exchange_kernel,
        out_shape=[pltpu.VMEM(shape, F32) for shape in OUTPUTS + BETWEEN],
        in_specs=[pl.BlockSpec(memory_space=pltpu.HBM)],
        out_specs=[vmem] * len(OUTPUTS + BETWEEN),
        scratch_shapes=[
            pltpu.VMEM((TILES + 2, ROWS, 128), F32),
            pltpu.VMEM((2, 128, 128), F32),
            columns,
            columns,
            pltpu.VMEM((TILES, ROWS, 128), F32),
            pltpu.VMEM((2, 2, TILES, HALO, 128), F32),
            near(MOST),
            near(MOST),
            pltpu.SemaphoreType.DMA((2 * len(SPANS) + 1,)),
            pltpu.SemaphoreType.DMA((5,)),
            pltpu.SemaphoreType.DMA((11,)),
        ],
        compiler_params=pltpu.CompilerParams(collective_id=0, has_side_effects=True, vmem_limit_bytes=46 << 20),
        name="exchange",
    )(x)
    return tuple(
        pl.pallas_call(
            store_kernel,
            out_shape=[jax.ShapeDtypeStruct(shape, F32) for shape in OUTPUTS],
            in_specs=[vmem] * len(OUTPUTS + BETWEEN),
            out_specs=[anywhere] * 3,
            scratch_shapes=[
                pltpu.VMEM((2, 2, HALO, 128), F32),
                [pltpu.VMEM((2, ROWS + 2 * pad_of(s), 128), F32) for s in LAGS],
                near(2),
                near(2),
                pltpu.VMEM((4, 2, ROWS, 128), F32),
                pltpu.SemaphoreType.DMA((3,)),
            ],
            compiler_params=pltpu.CompilerParams(vmem_limit_bytes=16 << 20),
            name="store",
        )(*results)
    )


def solution(mesh):
    in_specs = (P("lat", "lon"),)
    out_specs = (P("lat", "lon"), P(None, "lat", "lon"), P("lat", "lon"))
    return jax.shard_map(local, mesh=mesh, in_specs=in_specs, out_specs=out_specs, check_vma=False)
```
